32 devices in a mesh: sweep: 1 (over z), data: 4 (over y), ent: 8 (over x, core).
Axes of the slice: x: 4, y: 4, z: 1, core: 2. Of those that a mesh axis runs over, the one named last changes fastest.
The devices are a block of a 4x4x8 slice.
Arguments:
- ent_table: float32 [65536, 200], P(('sweep', 'ent'))
- ent_state: float32 [65536], P(('sweep', 'ent'))
- rel_table: float32 [11, 200], P('sweep')
- head_idx: int32 [8, 8, 8192], P(('sweep', 'ent'), None, 'data')
- tail_idx: int32 [8, 8, 8192], P(('sweep', 'ent'), None, 'data')
- rel_idx: int32 [8, 8, 8192], P(('sweep', 'ent'), None, 'data')
- edge_mask: int32 [8, 8, 8192], P(('sweep', 'ent'), None, 'data')
- neg_idx: int32 [8, 8, 768], P(('sweep', 'ent'))
Outputs:
- output 1: float32 [65536, 200], P(('sweep', 'ent'))
- output 2: float32 [65536], P(('sweep', 'ent'))
- output 3: float32 [11, 200], P('sweep')
- output 4: float32 [8, 8], P(('sweep', 'ent'))
All inputs are finite; a program needn't handle non-finite values.
Results may differ from the reference program's by a relative error of at most 0.001.
Values are sent between devices in bfloat16 or wider.
A program may use at most 768 MiB of HBM per device.

```python
import jax
import jax.numpy as jnp
from jax import lax

ENT_GROUP = 8
DATA_REPS = 4
ROWS_DEV = 8192
EDGES_DEV = 2048
NEG_COUNT = 768
EMBED_DIM = 200
REL_COUNT = 11
HOT_IDS = 16

TOTAL_ROWS = ENT_GROUP * ROWS_DEV
BUCKET_EDGES = DATA_REPS * EDGES_DEV
LR_SCALE = 0.2
EPSILON = 1e-8


def draw_edges(edge_key):
    subkeys = jax.random.split(edge_key, 14)
    edge_shape = (ENT_GROUP, ENT_GROUP, BUCKET_EDGES)
    hot_ent = jax.random.randint(subkeys[0], (ENT_GROUP, HOT_IDS), 0, ROWS_DEV)
    hot_rel = jax.random.randint(subkeys[1], (HOT_IDS,), 0, REL_COUNT)
    group_ids = jnp.arange(ENT_GROUP)
    tail_group = (group_ids[:, None] + group_ids[None, :]) % ENT_GROUP
    head_hot = jnp.broadcast_to(hot_ent[:, None, :], (ENT_GROUP, ENT_GROUP, HOT_IDS))
    tail_hot = hot_ent[tail_group]

    def pick_rows(key_use, key_slot, key_uni, hot_rows):
        use_hot = jax.random.randint(key_use, edge_shape, 0, 4) == 0
        hot_slot = jax.random.randint(key_slot, edge_shape, 0, HOT_IDS)
        hot_pick = jnp.take_along_axis(hot_rows, hot_slot, axis=2)
        uni_pick = jax.random.randint(key_uni, edge_shape, 0, ROWS_DEV)
        return jnp.where(use_hot, hot_pick, uni_pick)

    head_idx = pick_rows(subkeys[2], subkeys[3], subkeys[4], head_hot)
    tail_idx = pick_rows(subkeys[5], subkeys[6], subkeys[7], tail_hot)
    rel_use = jax.random.randint(subkeys[8], edge_shape, 0, 2) == 0
    rel_slot = jax.random.randint(subkeys[9], edge_shape, 0, HOT_IDS)
    rel_uni = jax.random.randint(subkeys[10], edge_shape, 0, REL_COUNT)
    rel_idx = jnp.where(rel_use, hot_rel[rel_slot], rel_uni)
    keep_level = jax.random.randint(subkeys[11], (ENT_GROUP, ENT_GROUP, 1), 1, 17)
    edge_mask = (jax.random.randint(subkeys[12], edge_shape, 0, 16) < keep_level).astype(jnp.int32)
    neg_idx = jax.random.randint(subkeys[13], (ENT_GROUP, ENT_GROUP, NEG_COUNT), 0, ROWS_DEV)
    head_idx = head_idx.at[:, :, 0].set(ROWS_DEV - 1)
    tail_idx = tail_idx.at[:, :, 0].set(ROWS_DEV - 1)
    neg_idx = neg_idx.at[:, :, 0].set(ROWS_DEV - 1)
    rel_idx = rel_idx.at[:, :, 0].set(REL_COUNT - 1)
    return head_idx, tail_idx, rel_idx, edge_mask, neg_idx


def setup_inputs(seed: int = 0, part: int = 0) -> dict:
    part_key = jax.random.fold_in(jax.random.key(seed), part)
    subkeys = jax.random.split(part_key, 4)
    emb_scale = EMBED_DIM ** -0.25
    ent_table = jax.random.normal(subkeys[0], (TOTAL_ROWS, EMBED_DIM), jnp.float32) * emb_scale
    ent_state = jax.random.uniform(subkeys[1], (TOTAL_ROWS,), jnp.float32, 0.01, 0.1) * EMBED_DIM ** -0.5
    rel_table = jax.random.normal(subkeys[2], (REL_COUNT, EMBED_DIM), jnp.float32) * 0.7
    head_idx, tail_idx, rel_idx, edge_mask, neg_idx = draw_edges(subkeys[3])
    return {'ent_table': ent_table, 'ent_state': ent_state, 'rel_table': rel_table, 'head_idx': head_idx, 'tail_idx': tail_idx, 'rel_idx': rel_idx, 'edge_mask': edge_mask, 'neg_idx': neg_idx}


def adagrad(param_rows, accum_rows, grad_rows, learn_rate):
    accum_new = accum_rows + jnp.mean(grad_rows * grad_rows, axis=-1)
    step_rows = grad_rows / jnp.sqrt(accum_new + EPSILON)[..., None]
    return param_rows - learn_rate * step_rows, accum_new


def bucket_terms(head_rows, rel_rows, tail_bf, neg_bf, weight):
    half_dim = head_rows.shape[1] // 2
    re_h = head_rows[:, :half_dim]
    im_h = head_rows[:, half_dim:]
    re_r = rel_rows[:, :half_dim]
    im_r = rel_rows[:, half_dim:]
    query_vec = jnp.concatenate([re_h * re_r - im_h * im_r, re_h * im_r + im_h * re_r], axis=1)
    query_bf = query_vec.astype(jnp.bfloat16)
    query_wide = query_bf.astype(jnp.float32)
    tail_wide = tail_bf.astype(jnp.float32)
    pos_score = jnp.sum(query_wide * tail_wide, axis=1)
    neg_score = jnp.dot(query_bf, neg_bf.T, preferred_element_type=jnp.float32)
    top_score = jnp.maximum(jnp.max(neg_score, axis=1), pos_score)
    pos_exp = jnp.exp(pos_score - top_score)
    neg_exp = jnp.exp(neg_score - top_score[:, None])
    exp_total = pos_exp + jnp.sum(neg_exp, axis=1)
    log_total = top_score + jnp.log(exp_total)
    loss_sum = jnp.sum(weight * (log_total - pos_score))
    d_pos = weight * (pos_exp / exp_total - 1.0)
    d_neg = ((weight / exp_total)[:, None] * neg_exp).astype(jnp.bfloat16)
    grad_query = d_pos[:, None] * tail_wide + jnp.dot(d_neg, neg_bf, preferred_element_type=jnp.float32)
    grad_tail = d_pos[:, None] * query_wide
    grad_neg = jnp.dot(d_neg.T, query_bf, preferred_element_type=jnp.float32)
    re_g = grad_query[:, :half_dim]
    im_g = grad_query[:, half_dim:]
    grad_head = jnp.concatenate([re_g * re_r + im_g * im_r, im_g * re_r - re_g * im_r], axis=1)
    grad_rel = jnp.concatenate([re_g * re_h + im_g * im_h, im_g * re_h - re_g * im_h], axis=1)
    return loss_sum, grad_head, grad_rel, grad_tail, grad_neg


def reference(ent_table, ent_state, rel_table, head_idx, tail_idx, rel_idx, edge_mask, neg_idx):
    groups = head_idx.shape[0]
    part_rows = ent_table.shape[0] // groups
    emb_width = ent_table.shape[1]
    rel_rows = rel_table.shape[0]
    bucket_edges = head_idx.shape[2]
    share_edges = bucket_edges // DATA_REPS
    learn_rate = LR_SCALE * emb_width ** -0.25
    pair_ids = jnp.arange(groups * DATA_REPS)

    def one_pass(pass_carry, step_idx):
        table_now, state_now, rel_now, rel_state = pass_carry
        table_bf = table_now.astype(jnp.bfloat16)

        def one_share(grad_acc, pair_id):
            ent_grad, rel_grad = grad_acc
            group_id = pair_id // DATA_REPS
            edge_start = (pair_id % DATA_REPS) * share_edges
            tail_base = ((group_id + step_idx) % groups) * part_rows
            h_ids = lax.dynamic_slice_in_dim(head_idx[group_id, step_idx], edge_start, share_edges) + group_id * part_rows
            t_ids = lax.dynamic_slice_in_dim(tail_idx[group_id, step_idx], edge_start, share_edges) + tail_base
            r_ids = lax.dynamic_slice_in_dim(rel_idx[group_id, step_idx], edge_start, share_edges)
            weight = lax.dynamic_slice_in_dim(edge_mask[group_id, step_idx], edge_start, share_edges).astype(jnp.float32)
            n_ids = neg_idx[group_id, step_idx] + tail_base
            loss_sum, g_head, g_rel, g_tail, g_neg = bucket_terms(table_now[h_ids], rel_now[r_ids], table_bf[t_ids], table_bf[n_ids], weight)
            ent_grad = ent_grad.at[h_ids].add(g_head).at[t_ids].add(g_tail).at[n_ids].add(g_neg)
            rel_grad = rel_grad.at[r_ids].add(g_rel)
            return (ent_grad, rel_grad), loss_sum

        share_init = (jnp.zeros_like(table_now), jnp.zeros_like(rel_now))
        grads_end, share_loss = lax.scan(one_share, share_init, pair_ids)
        ent_grad, rel_grad = grads_end
        table_now, state_now = adagrad(table_now, state_now, ent_grad, learn_rate)
        rel_now, rel_state = adagrad(rel_now, rel_state, rel_grad, learn_rate)
        bucket_loss = share_loss.reshape(groups, DATA_REPS).sum(axis=1) / bucket_edges
        return (table_now, state_now, rel_now, rel_state), bucket_loss

    pass_init = (ent_table, ent_state, rel_table, jnp.zeros((rel_rows,), jnp.float32))
    pass_end, losses = lax.scan(one_pass, pass_init, jnp.arange(groups))
    return pass_end[0], pass_end[1], pass_end[2], losses.T
```

```python
import functools

import jax
import jax.numpy as jnp
from jax import lax
from jax.experimental import pallas as pl
from jax.experimental.pallas import tpu as pltpu
from jax.sharding import PartitionSpec as P

LR_SCALE = 0.2
EPSILON = 1e-8
LANES = 128
EDGE_BLOCK = 256
GATHER_UNROLL = 16
SYNC_CHUNKS = 2
VMEM_LIMIT = 60 * 1024 * 1024
MESH = pl.DeviceIdType.MESH
VM = pltpu.VMEM
F32 = jnp.float32
BF16 = jnp.bfloat16


def interleave(table):
    rows, width = table.shape
    half = width // 2
    return jnp.pad(table.reshape(rows, 2, half), ((0, 0), (0, 0), (0, LANES - half))).reshape(rows * 2, LANES)


def deinterleave(table, width):
    rows = table.shape[0] // 2
    return table.reshape(rows, 2, LANES)[:, :, :width // 2].reshape(rows, width)


def pair(row):
    return pl.ds(pl.multiple_of(row * 2, 2), 2)


def gather_kernel(shift, h_ids, r_ids, t_ids, n_ids, table, rel, h_rows, r_rows, q_out, t_out, n_out, t_rows, n_rows):
    edges = t_out.shape[0]
    negs = n_out.shape[0]

    def gather_edges(step, _):
        base = step * GATHER_UNROLL
        for off in range(GATHER_UNROLL):
            at = base + off
            h_rows[pair(at), :] = table[pair(h_ids[shift, at]), :]
            r_rows[pair(at), :] = rel[pair(r_ids[shift, at]), :]
            t_rows[pair(at), :] = table[pair(t_ids[0, at]), :]
        return 0

    lax.fori_loop(0, edges // GATHER_UNROLL, gather_edges, 0)

    def gather_negs(step, _):
        base = step * GATHER_UNROLL
        for off in range(GATHER_UNROLL):
            at = base + off
            n_rows[pair(at), :] = table[pair(n_ids[0, at]), :]
        return 0

    lax.fori_loop(0, negs // GATHER_UNROLL, gather_negs, 0)

    def form(step, _):
        base = pl.multiple_of(step * LANES, LANES)
        rows = pl.ds(base, LANES)
        even = pl.ds(pl.multiple_of(2 * base, 2), LANES, stride=2)
        odd = pl.ds(2 * base + 1, LANES, stride=2)
        re_h, im_h = h_rows[even, :], h_rows[odd, :]
        re_r, im_r = r_rows[even, :], r_rows[odd, :]
        q_out[rows, 0:LANES] = (re_h * re_r - im_h * im_r).astype(BF16)
        q_out[rows, LANES:2 * LANES] = (re_h * im_r + im_h * re_r).astype(BF16)
        t_out[rows, 0:LANES] = t_rows[even, :].astype(BF16)
        t_out[rows, LANES:2 * LANES] = t_rows[odd, :].astype(BF16)
        return 0

    lax.fori_loop(0, edges // LANES, form, 0)

    def form_negs(step, _):
        base = pl.multiple_of(step * LANES, LANES)
        rows = pl.ds(base, LANES)
        n_out[rows, 0:LANES] = n_rows[pl.ds(pl.multiple_of(2 * base, 2), LANES, stride=2), :].astype(BF16)
        n_out[rows, LANES:2 * LANES] = n_rows[pl.ds(2 * base + 1, LANES, stride=2), :].astype(BF16)
        return 0

    lax.fori_loop(0, negs // LANES, form_negs, 0)


def bucket_kernel(shift, group, q_ref, t_ref, n_ref, w_ref, gq_ref, gt_ref, gn_ref, loss_ref, *scratch):
    edges = q_ref.shape[0]
    negs = n_ref.shape[0]
    steps = edges // EDGE_BLOCK
    if shift:
        gn_acc, q_got, gq_send, q_sems, gq_sems = scratch
        me = lax.axis_index('ent')
        ahead = lax.rem(me + shift, group)
        behind = lax.rem(me + group - shift, group)

        def block(step):
            return pl.ds(pl.multiple_of(step * EDGE_BLOCK, EDGE_BLOCK), EDGE_BLOCK)

        def q_copy(step):
            return pltpu.make_async_remote_copy(
                src_ref=q_ref.at[block(step), :], dst_ref=q_got.at[block(step), :],
                send_sem=q_sems.at[0, step], recv_sem=q_sems.at[1, step],
                device_id={'ent': ahead}, device_id_type=MESH)

        def gq_copy(step):
            return pltpu.make_async_remote_copy(
                src_ref=gq_send.at[block(step), :], dst_ref=gq_ref.at[block(step), :],
                send_sem=gq_sems.at[0, step], recv_sem=gq_sems.at[1, step],
                device_id={'ent': behind}, device_id_type=MESH)

        barrier = pltpu.get_barrier_semaphore()
        pl.semaphore_signal(barrier, inc=1, device_id={'ent': ahead}, device_id_type=MESH)
        pl.semaphore_signal(barrier, inc=1, device_id={'ent': behind}, device_id_type=MESH)
        pl.semaphore_wait(barrier, 2)
        for step in range(steps):
            q_copy(step).start()
        q_src, gq_dst = q_got, gq_send
    else:
        gn_acc, = scratch
        q_src, gq_dst = q_ref, gq_ref

    gn_acc[...] = jnp.zeros_like(gn_acc)
    eye = lax.broadcasted_iota(jnp.int32, (LANES, LANES), 0) == lax.broadcasted_iota(jnp.int32, (LANES, LANES), 1)
    per_block = EDGE_BLOCK // LANES

    def one_block(step, loss_acc):
        if shift:
            q_copy(step).wait_recv()
        base = pl.multiple_of(step * EDGE_BLOCK, EDGE_BLOCK)
        rows = pl.ds(base, EDGE_BLOCK)
        q = q_src[rows, :]
        t = t_ref[rows, :].astype(F32)
        q_wide = q.astype(F32)
        n = n_ref[...]
        w = jnp.concatenate(
            [jnp.sum(jnp.where(eye, w_ref[pl.ds(step * per_block + k, 1), :], 0.0), axis=1, keepdims=True) for k in range(per_block)], axis=0)
        pos = jnp.sum(q_wide * t, axis=1, keepdims=True)
        score = lax.dot_general(q, n, (((1,), (1,)), ((), ())), preferred_element_type=F32)
        top = jnp.maximum(jnp.max(score, axis=1, keepdims=True), pos)
        pos_exp = jnp.exp(pos - top)
        neg_exp = jnp.exp(score - top)
        total = pos_exp + jnp.sum(neg_exp, axis=1, keepdims=True)
        loss_acc = loss_acc + jnp.sum(w * (top + jnp.log(total) - pos), axis=0, keepdims=True)
        d_pos = w * (pos_exp / total - 1.0)
        d_neg = ((w / total) * neg_exp).astype(BF16)
        gq_dst[rows, :] = (d_pos * t + jnp.dot(d_neg, n, preferred_element_type=F32)).astype(gq_dst.dtype)
        g_tail = d_pos * q_wide
        gt_ref[pl.ds(pl.multiple_of(2 * base, 2), EDGE_BLOCK, stride=2), :] = g_tail[:, 0:LANES]
        gt_ref[pl.ds(2 * base + 1, EDGE_BLOCK, stride=2), :] = g_tail[:, LANES:2 * LANES]
        gn_acc[...] += lax.dot_general(q, d_neg, (((0,), (0,)), ((), ())), preferred_element_type=F32)
        if shift:
            gq_copy(step).start()
        return loss_acc

    loss = lax.fori_loop(0, steps, one_block, jnp.zeros((1, 1), F32))
    loss_ref[...] = jnp.broadcast_to(loss, loss_ref.shape)
    for half in range(2):
        gn_ref[pl.ds(half, negs, stride=2), :] = gn_acc[half * LANES:(half + 1) * LANES, :].T
    if shift:
        for step in range(steps):
            q_copy(step).wait_send()
            gq_copy(step).wait()


def scatter_kernel(shift, h_ids, t_ids, n_ids, r_ref, gq_ref, h_rows, r_rows, gt_ref, gn_ref, acc, grel, acc_b, acc_c, acc_d, gh):
    edges = gq_ref.shape[0]
    negs = gn_ref.shape[0] // 2
    table_rows = acc.shape[0]
    rel_pad = grel.shape[0] // 2

    zero_rows = 512

    def clear(step, _):
        rows = pl.ds(pl.multiple_of(step * zero_rows, zero_rows), zero_rows)
        for ref in (acc, acc_b, acc_c, acc_d):
            ref[rows, :] = jnp.zeros((zero_rows, LANES), F32)
        return 0

    lax.fori_loop(0, table_rows // zero_rows, clear, 0)

    def form(step, carry):
        rel_re, rel_im = carry
        base = pl.multiple_of(step * LANES, LANES)
        rows = pl.ds(base, LANES)
        even = pl.ds(pl.multiple_of(2 * base, 2), LANES, stride=2)
        odd = pl.ds(2 * base + 1, LANES, stride=2)
        re_g = gq_ref[rows, 0:LANES].astype(F32)
        im_g = gq_ref[rows, LANES:2 * LANES].astype(F32)
        re_r, im_r = r_rows[even, :], r_rows[odd, :]
        gh[even, :] = re_g * re_r + im_g * im_r
        gh[odd, :] = im_g * re_r - re_g * im_r
        re_h, im_h = h_rows[even, :], h_rows[odd, :]
        hot = (lax.broadcasted_iota(jnp.int32, (rel_pad, LANES), 0) == r_ref[pl.ds(step, 1), :]).astype(F32)
        rel_re = rel_re + jnp.dot(hot, re_g * re_h + im_g * im_h, precision=lax.Precision.HIGHEST, preferred_element_type=F32)
        rel_im = rel_im + jnp.dot(hot, im_g * re_h - re_g * im_h, precision=lax.Precision.HIGHEST, preferred_element_type=F32)
        return rel_re, rel_im

    zero = jnp.zeros((rel_pad, LANES), F32)
    rel_re, rel_im = lax.fori_loop(0, edges // LANES, form, (zero, zero))
    grel[pl.ds(0, rel_pad, stride=2), :] = rel_re
    grel[pl.ds(1, rel_pad, stride=2), :] = rel_im

    def add_edges(step, _):
        base = step * GATHER_UNROLL
        for off in range(0, GATHER_UNROLL, 2):
            at = base + off
            places = (pair(h_ids[shift, at]), pair(h_ids[shift, at + 1]), pair(t_ids[0, at]), pair(t_ids[0, at + 1]))
            refs = (acc, acc_b, acc_c, acc_d)
            terms = (gh[pair(at), :], gh[pair(at + 1), :], gt_ref[pair(at), :], gt_ref[pair(at + 1), :])
            sums = [ref[place, :] + term for ref, place, term in zip(refs, places, terms)]
            for ref, place, total in zip(refs, places, sums):
                ref[place, :] = total
        return 0

    lax.fori_loop(0, edges // GATHER_UNROLL, add_edges, 0)

    def add_negs(step, _):
        base = step * GATHER_UNROLL
        for off in range(0, GATHER_UNROLL, 4):
            at = base + off
            places = [pair(n_ids[0, at + k]) for k in range(4)]
            refs = (acc, acc_b, acc_c, acc_d)
            sums = [ref[place, :] + gn_ref[pair(at + k), :] for k, (ref, place) in enumerate(zip(refs, places))]
            for ref, place, total in zip(refs, places, sums):
                ref[place, :] = total
        return 0

    lax.fori_loop(0, negs // GATHER_UNROLL, add_negs, 0)

    def combine(step, _):
        rows = pl.ds(pl.multiple_of(step * zero_rows, zero_rows), zero_rows)
        acc[rows, :] = (acc[rows, :] + acc_b[rows, :]) + (acc_c[rows, :] + acc_d[rows, :])
        return 0

    lax.fori_loop(0, table_rows // zero_rows, combine, 0)


def update_kernel(width, learn_rate, groups, reps, acc_in, table_in, state_in, grel_in, rel_in, rel_state_in,
                  table_out, state_out, rel_out, rel_state_out,
                  first_send, first_got, plain_send, plain_got, merged_send, merged_got, work,
                  step_own, step_got, step_far, rel_x, rel_y, rel_send,
                  first_sems, plain_sems, merged_sems, own_sems, far_sems, rel_x_sems, rel_y_sems):
    me = lax.axis_index('data')
    ent = lax.axis_index('ent')
    peers = (lax.rem(me + 1, reps), lax.rem(me + reps - 1, reps))
    far = lax.rem(me + 2, reps)
    quarter = acc_in.shape[0] // reps
    half = quarter // 2
    chunk = half // SYNC_CHUNKS

    barrier = pltpu.get_barrier_semaphore()
    for off in range(1, reps):
        pl.semaphore_signal(barrier, inc=1, device_id={'data': lax.rem(me + off, reps)}, device_id_type=MESH)
    for off in range(1, groups):
        pl.semaphore_signal(barrier, inc=1, device_id={'ent': lax.rem(ent + off, groups)}, device_id_type=MESH)
    pl.semaphore_wait(barrier, reps + groups - 2)

    def remote(src, dst, sems, place, to):
        return pltpu.make_async_remote_copy(
            src_ref=src, dst_ref=dst, send_sem=sems.at[(0,) + place], recv_sem=sems.at[(1,) + place],
            device_id=to, device_id_type=MESH)

    rel_x[0] = grel_in[...]
    rel_send[...] = grel_in[...]
    x_copies = [remote(rel_send, rel_x.at[off], rel_x_sems, (off - 1,), {'ent': lax.rem(ent + off, groups)}) for off in range(1, groups)]
    for copy in x_copies:
        copy.start()

    def rows_of(owner, which, k):
        return pl.ds(pl.multiple_of(owner * quarter + which * half + k * chunk, chunk), chunk)

    def at_chunk(k):
        return pl.ds(k * chunk, chunk)

    first, plain, merged = {}, {}, {}
    for k in range(SYNC_CHUNKS):
        for side in range(2):
            first_send[side, at_chunk(k), :] = acc_in[rows_of(far, side, k), :].astype(BF16)
            first[side, k] = remote(first_send.at[side, at_chunk(k), :], first_got.at[side, at_chunk(k), :], first_sems, (side, k), {'data': peers[side]})
            first[side, k].start()
    for k in range(SYNC_CHUNKS):
        for side in range(2):
            plain_send[side, at_chunk(k), :] = acc_in[rows_of(peers[side], 1 - side, k), :].astype(BF16)
            plain[side, k] = remote(plain_send.at[side, at_chunk(k), :], plain_got.at[side, at_chunk(k), :], plain_sems, (side, k), {'data': peers[side]})
            plain[side, k].start()
    for k in range(SYNC_CHUNKS):
        for side in range(2):
            first[side, k].wait_recv()
            merged_send[side, at_chunk(k), :] = (first_got[side, at_chunk(k), :].astype(F32) + acc_in[rows_of(peers[side], side, k), :]).astype(BF16)
            merged[side, k] = remote(merged_send.at[side, at_chunk(k), :], merged_got.at[side, at_chunk(k), :], merged_sems, (side, k), {'data': peers[side]})
            merged[side, k].start()

    for copy in x_copies:
        copy.wait()
    total = rel_x[lax.rem(ent, groups)]
    for src in range(1, groups):
        total = total + rel_x[lax.rem(ent + groups - src, groups)]
    rel_y[0] = total
    rel_send[...] = total
    y_copies = [remote(rel_send, rel_y.at[off], rel_y_sems, (off - 1,), {'data': lax.rem(me + off, reps)}) for off in range(1, reps)]
    for copy in y_copies:
        copy.start()

    own = {}
    for k in range(SYNC_CHUNKS):
        for which in range(2):
            merged[which, k].wait_recv()
            plain[1 - which, k].wait_recv()
            work[...] = acc_in[rows_of(me, which, k), :] + (merged_got[which, at_chunk(k), :].astype(F32) + plain_got[1 - which, at_chunk(k), :].astype(F32))
            n = chunk // 2
            re_g, im_g = work[pl.ds(0, n, stride=2), :], work[pl.ds(1, n, stride=2), :]
            places = pl.ds(which * (half // 2) + k * n, n)
            state = state_in[places, :] + jnp.sum(re_g * re_g + im_g * im_g, axis=1, keepdims=True) / width
            state_out[places, :] = state
            scale = learn_rate / jnp.sqrt(state + EPSILON)
            work[pl.ds(0, n, stride=2), :] = re_g * scale
            work[pl.ds(1, n, stride=2), :] = im_g * scale
            step_own[which, at_chunk(k), :] = work[...].astype(BF16)
            for side in range(2):
                own[side, which, k] = remote(step_own.at[which, at_chunk(k), :], step_got.at[side, which, at_chunk(k), :], own_sems, (side, which, k), {'data': peers[side]})
                own[side, which, k].start()

    spread = {}
    for k in range(SYNC_CHUNKS):
        for which in range(2):
            for side in range(2):
                own[side, which, k].wait_recv()
                if side == which:
                    spread[side, k] = remote(step_got.at[side, which, at_chunk(k), :], step_far.at[side, at_chunk(k), :], far_sems, (side, k), {'data': peers[side]})
                    spread[side, k].start()
            for owner, ref in ((me, step_own.at[which]), (peers[1], step_got.at[0, which]), (peers[0], step_got.at[1, which])):
                rows = rows_of(owner, which, k)
                table_out[rows, :] = table_in[rows, :] - ref[at_chunk(k), :].astype(F32)

    for copy in y_copies:
        copy.wait()
    total = rel_y[lax.rem(me, reps)]
    for src in range(1, reps):
        total = total + rel_y[lax.rem(me + reps - src, reps)]
    rel_send[...] = total
    rel_rows = rel_send.shape[0] // 2
    re_g, im_g = rel_send[pl.ds(0, rel_rows, stride=2), :], rel_send[pl.ds(1, rel_rows, stride=2), :]
    state = rel_state_in[...] + jnp.sum(re_g * re_g + im_g * im_g, axis=1, keepdims=True) / width
    rel_state_out[...] = state
    scale = learn_rate / jnp.sqrt(state + EPSILON)
    rel_out[pl.ds(0, rel_rows, stride=2), :] = rel_in[pl.ds(0, rel_rows, stride=2), :] - re_g * scale
    rel_out[pl.ds(1, rel_rows, stride=2), :] = rel_in[pl.ds(1, rel_rows, stride=2), :] - im_g * scale

    for k in range(SYNC_CHUNKS):
        for side in range(2):
            spread[side, k].wait_recv()
            rows = rows_of(far, side, k)
            table_out[rows, :] = table_in[rows, :] - step_far[side, at_chunk(k), :].astype(F32)
    for group_of in (first, plain, merged, own, spread):
        for copy in group_of.values():
            copy.wait_send()


def solution(mesh):
    groups = mesh.shape['ent']
    reps = mesh.shape['data']
    row_spec = P(('sweep', 'ent'), None)
    edge_spec = P(('sweep', 'ent'), None, 'data')
    vmem = pl.BlockSpec(memory_space=VM)

    def device_fn(ent_table, ent_state, rel_table, head_idx, tail_idx, rel_idx, edge_mask, neg_idx):
        part_rows, width = ent_table.shape
        rel_count = rel_table.shape[0]
        edges = head_idx.shape[2]
        negs = neg_idx.shape[2]
        bucket_edges = edges * reps
        learn_rate = LR_SCALE * width ** -0.25
        rel_pad = -(-rel_count // 8) * 8
        quarter = part_rows // reps
        me = lax.axis_index('data')
        ent = lax.axis_index('ent')

        packed = jnp.concatenate([tail_idx[0], edge_mask[0], neg_idx[0]], axis=1)
        moved = [packed[0:1]]
        for shift in range(1, groups):
            moved.append(lax.ppermute(packed[shift:shift + 1], 'ent', [(src, (src + shift) % groups) for src in range(groups)]))

        h_all = head_idx[0]
        r_all = rel_idx[0]
        r_vec = rel_idx.reshape(groups, edges // LANES, LANES)

        table = interleave(ent_table)
        rel = interleave(jnp.pad(rel_table, ((0, rel_pad - rel_count), (0, 0))))
        rel_state = jnp.zeros((rel_pad, LANES), F32)
        state = jnp.broadcast_to(lax.dynamic_slice_in_dim(ent_state, me * quarter, quarter)[:, None], (quarter, LANES))
        losses = []

        smem = pl.BlockSpec(memory_space=pltpu.SMEM)
        params = pltpu.CompilerParams(vmem_limit_bytes=VMEM_LIMIT)
        for shift in range(groups):
            got = moved[shift]
            t_ids = got[:, :edges]
            n_ids = got[:, 2 * edges:]
            weight = got[:, edges:2 * edges].reshape(edges // LANES, LANES).astype(F32)

            h_rows, r_rows, q, t, n = pl.pallas_call(
                functools.partial(gather_kernel, shift),
                out_shape=[jax.ShapeDtypeStruct((2 * edges, LANES), F32)] * 2
                + [jax.ShapeDtypeStruct((edges, 2 * LANES), BF16)] * 2 + [jax.ShapeDtypeStruct((negs, 2 * LANES), BF16)],
                in_specs=[smem] * 4 + [vmem] * 2,
                out_specs=[vmem] * 5,
                scratch_shapes=[VM((2 * edges, LANES), F32), VM((2 * negs, LANES), F32)],
                compiler_params=params, name='gather_rows',
            )(h_all, r_all, t_ids, n_ids, table, rel)

            scratch = [VM((2 * LANES, negs), F32)]
            if shift:
                steps = edges // EDGE_BLOCK
                scratch += [VM((edges, 2 * LANES), BF16), VM((edges, 2 * LANES), BF16),
                            pltpu.SemaphoreType.DMA((2, steps)), pltpu.SemaphoreType.DMA((2, steps))]
            g_q, g_t, g_n, loss = pl.pallas_call(
                functools.partial(bucket_kernel, shift, groups),
                out_shape=[jax.ShapeDtypeStruct((edges, 2 * LANES), BF16 if shift else F32), jax.ShapeDtypeStruct((2 * edges, LANES), F32),
                           jax.ShapeDtypeStruct((2 * negs, LANES), F32), jax.ShapeDtypeStruct((8, LANES), F32)],
                in_specs=[vmem] * 4, out_specs=[vmem] * 4, scratch_shapes=scratch,
                compiler_params=pltpu.CompilerParams(vmem_limit_bytes=VMEM_LIMIT, collective_id=0, has_side_effects=True) if shift else params,
                name='bucket',
            )(q, t, n, weight)
            losses.append(loss[0, 0])

            acc, g_rel = pl.pallas_call(
                functools.partial(scatter_kernel, shift),
                out_shape=[jax.ShapeDtypeStruct((2 * part_rows, LANES), F32), jax.ShapeDtypeStruct((2 * rel_pad, LANES), F32)],
                in_specs=[smem] * 3 + [vmem] * 6, out_specs=[vmem] * 2,
                scratch_shapes=[VM((2 * part_rows, LANES), F32)] * 3 + [VM((2 * edges, LANES), F32)],
                compiler_params=params, name='scatter_rows',
            )(h_all, t_ids, n_ids, r_vec[shift], g_q, h_rows, r_rows, g_t, g_n)

            half = (2 * part_rows) // reps // 2
            block = VM((2, half, LANES), BF16)
            sems = pltpu.SemaphoreType.DMA
            table, state, rel, rel_state = pl.pallas_call(
                functools.partial(update_kernel, width, learn_rate, groups, reps),
                out_shape=[jax.ShapeDtypeStruct(table.shape, F32), jax.ShapeDtypeStruct(state.shape, F32),
                           jax.ShapeDtypeStruct(rel.shape, F32), jax.ShapeDtypeStruct(rel_state.shape, F32)],
                in_specs=[vmem] * 6, out_specs=[vmem] * 4,
                scratch_shapes=[block] * 6 + [VM((half // SYNC_CHUNKS, LANES), F32), block, VM((2, 2, half, LANES), BF16), block,
                                              VM((groups, 2 * rel_pad, LANES), F32), VM((reps, 2 * rel_pad, LANES), F32), VM((2 * rel_pad, LANES), F32),
                                              sems((2, 2, SYNC_CHUNKS)), sems((2, 2, SYNC_CHUNKS)), sems((2, 2, SYNC_CHUNKS)),
                                              sems((2, 2, 2, SYNC_CHUNKS)), sems((2, 2, SYNC_CHUNKS)), sems((2, groups - 1)), sems((2, reps - 1))],
                compiler_params=pltpu.CompilerParams(vmem_limit_bytes=VMEM_LIMIT, collective_id=1, has_side_effects=True), name='update',
            )(acc, table, state, g_rel, rel, rel_state)

        ent_out = deinterleave(table, width)
        state_out = lax.all_gather(state[:, 0], 'data', tiled=True)
        rel_out = deinterleave(rel, width)[:rel_count]
        mine = jnp.stack(losses)
        home = lax.rem(ent + groups - jnp.arange(groups), groups)
        spread = jnp.zeros((groups, groups), F32).at[home, jnp.arange(groups)].set(mine)
        bucket_loss = lax.psum(spread, ('data', 'ent'))
        loss_out = lax.dynamic_slice_in_dim(bucket_loss, ent, 1) / bucket_edges
        return ent_out, state_out, rel_out, loss_out

    return jax.shard_map(device_fn, mesh=mesh, in_specs=(row_spec, P(('sweep', 'ent')), P('sweep', None), edge_spec, edge_spec, edge_spec, edge_spec, P(('sweep', 'ent'), None, None)), out_specs=(row_spec, P(('sweep', 'ent')), P('sweep', None), row_spec), check_vma=False)
```

```python
import functools

import jax
import jax.numpy as jnp
from jax import lax
from jax.experimental import pallas as pl
from jax.experimental.pallas import tpu as pltpu
from jax.sharding import PartitionSpec as P

LR_SCALE = 0.2
EPSILON = 1e-8
LANES = 128
EDGE_BLOCK = 256
GATHER_UNROLL = 16
SYNC_CHUNKS = 2
VMEM_LIMIT = 60 * 1024 * 1024
MESH = pl.DeviceIdType.MESH
VM = pltpu.VMEM
F32 = jnp.float32
BF16 = jnp.bfloat16


def interleave(table):
    rows, width = table.shape
    half = width // 2
    return jnp.pad(table.reshape(rows, 2, half), ((0, 0), (0, 0), (0, LANES - half))).reshape(rows * 2, LANES)


def deinterleave(table, width):
    rows = table.shape[0] // 2
    return table.reshape(rows, 2, LANES)[:, :, :width // 2].reshape(rows, width)


def pair(row):
    return pl.ds(pl.multiple_of(row * 2, 2), 2)


def load_kernel(half, table_t, table, staged):
    width, cols = table_t.shape
    staged[0:width, :] = table_t[...]
    staged[width:2 * LANES, :] = jnp.zeros((2 * LANES - width, cols), F32)
    lane = lax.broadcasted_iota(jnp.int32, (LANES, LANES), 1)
    for at in range(0, cols, LANES):
        low = staged[0:LANES, at:at + LANES].T
        high = staged[LANES:2 * LANES, at:at + LANES].T
        table[pl.ds(2 * at, LANES, stride=2), :] = jnp.where(lane < half, low, 0.0)
        moved = jnp.where(lane < LANES - half, pltpu.roll(low, LANES - half, 1), pltpu.roll(high, LANES - half, 1))
        table[pl.ds(2 * at + 1, LANES, stride=2), :] = jnp.where(lane < half, moved, 0.0)


def store_kernel(half, table, table_t):
    width, cols = table_t.shape
    lane = lax.broadcasted_iota(jnp.int32, (LANES, LANES), 1)
    for at in range(0, cols, LANES):
        re = table[pl.ds(2 * at, LANES, stride=2), :]
        moved = pltpu.roll(table[pl.ds(2 * at + 1, LANES, stride=2), :], half, 1)
        table_t[0:LANES, at:at + LANES] = jnp.where(lane < half, re, moved).T
        table_t[LANES:width, at:at + LANES] = moved.T[0:width - LANES, :]


def bucket_kernel(shift, group, h_ids, r_ids, tail_ids, table, rel, r_vec, tail_vec,
                  gh_ref, gt_ref, gn_ref, grel_ref, loss_ref,
                  h_rows, r_rows, t_rows, n_rows, q_own, n_bf, gn_acc, *scratch):
    edges = q_own.shape[0]
    negs = n_bf.shape[0]
    rel_pad = grel_ref.shape[0] // 2
    steps = edges // EDGE_BLOCK

    def block(step):
        return pl.ds(pl.multiple_of(step * EDGE_BLOCK, EDGE_BLOCK), EDGE_BLOCK)

    def halves(base, count):
        return pl.ds(pl.multiple_of(2 * base, 2), count, stride=2), pl.ds(2 * base + 1, count, stride=2)

    if shift:
        q_got, gq_send, gq_got, loss_send, q_sems, gq_sems, loss_sems = scratch
        me = lax.axis_index('ent')
        ahead = lax.rem(me + shift, group)
        behind = lax.rem(me + group - shift, group)

        def q_copy(step):
            return pltpu.make_async_remote_copy(
                src_ref=q_own.at[block(step), :], dst_ref=q_got.at[block(step), :],
                send_sem=q_sems.at[0, step], recv_sem=q_sems.at[1, step],
                device_id={'ent': ahead}, device_id_type=MESH)

        def gq_copy(step):
            return pltpu.make_async_remote_copy(
                src_ref=gq_send.at[block(step), :], dst_ref=gq_got.at[block(step), :],
                send_sem=gq_sems.at[0, step], recv_sem=gq_sems.at[1, step],
                device_id={'ent': behind}, device_id_type=MESH)

        barrier = pltpu.get_barrier_semaphore()
        pl.semaphore_signal(barrier, inc=1, device_id={'ent': ahead}, device_id_type=MESH)
        pl.semaphore_signal(barrier, inc=1, device_id={'ent': behind}, device_id_type=MESH)
        pl.semaphore_wait(barrier, 2)
        q_src, gq_src, gq_dst = q_got, gq_got, gq_send
    else:
        gq_got, = scratch
        q_src, gq_src, gq_dst = q_own, gq_got, gq_got

    def ask(step, _):
        def gather(part, _):
            base = step * EDGE_BLOCK + part * GATHER_UNROLL
            for off in range(GATHER_UNROLL):
                at = base + off
                h_rows[pair(at), :] = table[h_ids[shift, at]]
                r_rows[pair(at), :] = rel[r_ids[shift, at]]
            return 0

        lax.fori_loop(0, EDGE_BLOCK // GATHER_UNROLL, gather, 0)
        rows = block(step)
        even, odd = halves(step * EDGE_BLOCK, EDGE_BLOCK)
        re_h, im_h = h_rows[even, :], h_rows[odd, :]
        re_r, im_r = r_rows[even, :], r_rows[odd, :]
        q_own[rows, 0:LANES] = (re_h * re_r - im_h * im_r).astype(BF16)
        q_own[rows, LANES:2 * LANES] = (re_h * im_r + im_h * re_r).astype(BF16)
        if shift:
            q_copy(step).start()
        return 0

    lax.fori_loop(0, steps, ask, 0)

    def gather_negs(part, _):
        for off in range(GATHER_UNROLL):
            at = part * GATHER_UNROLL + off
            n_rows[pair(at), :] = table[tail_ids[0, 2 * edges + at]]
        return 0

    lax.fori_loop(0, negs // GATHER_UNROLL, gather_negs, 0)
    n_even, n_odd = halves(0, negs)
    n_bf[:, 0:LANES] = n_rows[n_even, :].astype(BF16)
    n_bf[:, LANES:2 * LANES] = n_rows[n_odd, :].astype(BF16)

    def gather_tails(part, _):
        for off in range(GATHER_UNROLL):
            at = part * GATHER_UNROLL + off
            t_rows[pair(at), :] = table[tail_ids[0, at]]
        return 0

    lax.fori_loop(0, edges // GATHER_UNROLL, gather_tails, 0)

    gn_acc[...] = jnp.zeros_like(gn_acc)
    eye = lax.broadcasted_iota(jnp.int32, (LANES, LANES), 0) == lax.broadcasted_iota(jnp.int32, (LANES, LANES), 1)
    per_block = EDGE_BLOCK // LANES

    def answer(step, loss_acc):
        if shift:
            q_copy(step).wait_recv()
        rows = block(step)
        even, odd = halves(step * EDGE_BLOCK, EDGE_BLOCK)
        q = q_src[rows, :]
        t = jnp.concatenate([t_rows[even, :].astype(BF16), t_rows[odd, :].astype(BF16)], axis=1).astype(F32)
        q_wide = q.astype(F32)
        n = n_bf[...]
        masks = [tail_vec[0:1, pl.ds(pl.multiple_of(edges + step * EDGE_BLOCK + k * LANES, LANES), LANES)].astype(F32) for k in range(per_block)]
        w = jnp.concatenate([jnp.sum(jnp.where(eye, mask, 0.0), axis=1, keepdims=True) for mask in masks], axis=0)
        pos = jnp.sum(q_wide * t, axis=1, keepdims=True)
        score = lax.dot_general(q, n, (((1,), (1,)), ((), ())), preferred_element_type=F32)
        top = jnp.maximum(jnp.max(score, axis=1, keepdims=True), pos)
        pos_exp = jnp.exp(pos - top)
        neg_exp = jnp.exp(score - top)
        total = pos_exp + jnp.sum(neg_exp, axis=1, keepdims=True)
        loss_acc = loss_acc + jnp.sum(w * (top + jnp.log(total) - pos), axis=0, keepdims=True)
        d_pos = w * (pos_exp / total - 1.0)
        d_neg = ((w / total) * neg_exp).astype(BF16)
        gq_dst[rows, :] = (d_pos * t + jnp.dot(d_neg, n, preferred_element_type=F32)).astype(gq_dst.dtype)
        g_tail = d_pos * q_wide
        gt_ref[even, :] = g_tail[:, 0:LANES]
        gt_ref[odd, :] = g_tail[:, LANES:2 * LANES]
        gn_acc[...] += lax.dot_general(q, d_neg, (((0,), (0,)), ((), ())), preferred_element_type=F32)
        if shift:
            gq_copy(step).start()
        return loss_acc

    loss = lax.fori_loop(0, steps, answer, jnp.zeros((1, 1), F32))
    if shift:
        loss_send[...] = jnp.broadcast_to(loss, loss_send.shape)
        loss_copy = pltpu.make_async_remote_copy(
            src_ref=loss_send, dst_ref=loss_ref, send_sem=loss_sems.at[0], recv_sem=loss_sems.at[1],
            device_id={'ent': behind}, device_id_type=MESH)
        loss_copy.start()
    else:
        loss_ref[...] = jnp.broadcast_to(loss, loss_ref.shape)
    for half in range(2):
        gn_ref[pl.ds(half, negs, stride=2), :] = gn_acc[half * LANES:(half + 1) * LANES, :].T

    def finish(step, carry):
        rel_re, rel_im = carry
        if shift:
            gq_copy(step).wait_recv()
        rows = block(step)
        even, odd = halves(step * EDGE_BLOCK, EDGE_BLOCK)
        re_g, im_g = gq_src[rows, 0:LANES].astype(F32), gq_src[rows, LANES:2 * LANES].astype(F32)
        re_r, im_r = r_rows[even, :], r_rows[odd, :]
        gh_ref[even, :] = re_g * re_r + im_g * im_r
        gh_ref[odd, :] = im_g * re_r - re_g * im_r
        re_h, im_h = h_rows[even, :], h_rows[odd, :]
        ids = r_vec[shift:shift + 1, pl.ds(pl.multiple_of(step * EDGE_BLOCK, EDGE_BLOCK), EDGE_BLOCK)]
        hot = (lax.broadcasted_iota(jnp.int32, (rel_pad, EDGE_BLOCK), 0) == ids).astype(F32)
        rel_re = rel_re + jnp.dot(hot, re_g * re_h + im_g * im_h, precision=lax.Precision.HIGHEST, preferred_element_type=F32)
        rel_im = rel_im + jnp.dot(hot, im_g * re_h - re_g * im_h, precision=lax.Precision.HIGHEST, preferred_element_type=F32)
        return rel_re, rel_im

    zero = jnp.zeros((rel_pad, LANES), F32)
    rel_re, rel_im = lax.fori_loop(0, steps, finish, (zero, zero))
    grel_ref[pl.ds(0, rel_pad, stride=2), :] = rel_re
    grel_ref[pl.ds(1, rel_pad, stride=2), :] = rel_im
    if shift:
        loss_copy.wait()

        def drain(step, _):
            q_copy(step).wait_send()
            gq_copy(step).wait_send()
            return 0

        lax.fori_loop(0, steps, drain, 0)


def scatter_kernel(shift, h_ids, tail_ids, gh, gt_ref, gn_ref, acc, acc_b, acc_c, acc_d):
    edges = gh.shape[0] // 2
    negs = gn_ref.shape[0] // 2
    table_rows = acc.shape[0]

    zero_rows = 512

    def clear(step, _):
        rows = pl.ds(pl.multiple_of(step * zero_rows, zero_rows), zero_rows)
        for ref in (acc, acc_b, acc_c, acc_d):
            ref[rows, :] = jnp.zeros((zero_rows, LANES), F32)
        return 0

    lax.fori_loop(0, table_rows // zero_rows, clear, 0)

    def add_edges(step, _):
        base = step * GATHER_UNROLL
        for off in range(0, GATHER_UNROLL, 2):
            at = base + off
            places = (pair(h_ids[shift, at]), pair(h_ids[shift, at + 1]), pair(tail_ids[0, at]), pair(tail_ids[0, at + 1]))
            refs = (acc, acc_b, acc_c, acc_d)
            terms = (gh[pair(at), :], gh[pair(at + 1), :], gt_ref[pair(at), :], gt_ref[pair(at + 1), :])
            sums = [ref[place, :] + term for ref, place, term in zip(refs, places, terms)]
            for ref, place, total in zip(refs, places, sums):
                ref[place, :] = total
        return 0

    lax.fori_loop(0, edges // GATHER_UNROLL, add_edges, 0)

    def add_negs(step, _):
        base = step * GATHER_UNROLL
        for off in range(0, GATHER_UNROLL, 4):
            at = base + off
            places = [pair(tail_ids[0, 2 * edges + at + k]) for k in range(4)]
            refs = (acc, acc_b, acc_c, acc_d)
            sums = [ref[place, :] + gn_ref[pair(at + k), :] for k, (ref, place) in enumerate(zip(refs, places))]
            for ref, place, total in zip(refs, places, sums):
                ref[place, :] = total
        return 0

    lax.fori_loop(0, negs // GATHER_UNROLL, add_negs, 0)

    def combine(step, _):
        rows = pl.ds(pl.multiple_of(step * zero_rows, zero_rows), zero_rows)
        acc[rows, :] = (acc[rows, :] + acc_b[rows, :]) + (acc_c[rows, :] + acc_d[rows, :])
        return 0

    lax.fori_loop(0, table_rows // zero_rows, combine, 0)


def update_kernel(width, learn_rate, groups, reps, shift, bucket_edges, acc_in, table_in, state_in, grel_in, rel_in, rel_state_in, loss_in, losses_in,
                  table_out, state_out, rel_out, rel_state_out, losses_out, state_all,
                  first_send, first_got, plain_send, plain_got, merged_send, merged_got, work,
                  step_own, step_got, step_far, rel_x, rel_y, rel_send, rel_send_y, state_own,
                  first_sems, plain_sems, merged_sems, own_sems, far_sems, rel_x_sems, rel_y_sems, state_sems):
    me = lax.axis_index('data')
    ent = lax.axis_index('ent')
    peers = (lax.rem(me + 1, reps), lax.rem(me + reps - 1, reps))
    far = lax.rem(me + 2, reps)
    quarter = acc_in.shape[0] // reps
    half = quarter // 2
    chunk = half // SYNC_CHUNKS

    barrier = pltpu.get_barrier_semaphore()
    for off in range(1, reps):
        pl.semaphore_signal(barrier, inc=1, device_id={'data': lax.rem(me + off, reps)}, device_id_type=MESH)
    for off in range(1, groups):
        pl.semaphore_signal(barrier, inc=1, device_id={'ent': lax.rem(ent + off, groups)}, device_id_type=MESH)
    pl.semaphore_wait(barrier, reps + groups - 2)

    def remote(src, dst, sems, place, to):
        return pltpu.make_async_remote_copy(
            src_ref=src, dst_ref=dst, send_sem=sems.at[(0,) + place], recv_sem=sems.at[(1,) + place],
            device_id=to, device_id_type=MESH)

    rel_x[0] = grel_in[...]
    rel_send[...] = grel_in[...]
    x_copies = [remote(rel_send, rel_x.at[off], rel_x_sems, (off - 1,), {'ent': lax.rem(ent + off, groups)}) for off in range(1, groups)]
    for copy in x_copies:
        copy.start()

    def rows_of(owner, which, k):
        return pl.ds(pl.multiple_of(owner * quarter + which * half + k * chunk, chunk), chunk)

    def at_chunk(k):
        return pl.ds(k * chunk, chunk)

    first, plain, merged = {}, {}, {}
    for k in range(SYNC_CHUNKS):
        for side in range(2):
            first_send[side, at_chunk(k), :] = acc_in[rows_of(far, side, k), :].astype(BF16)
            first[side, k] = remote(first_send.at[side, at_chunk(k), :], first_got.at[side, at_chunk(k), :], first_sems, (side, k), {'data': peers[side]})
            first[side, k].start()
    for k in range(SYNC_CHUNKS):
        for side in range(2):
            plain_send[side, at_chunk(k), :] = acc_in[rows_of(peers[side], 1 - side, k), :].astype(BF16)
            plain[side, k] = remote(plain_send.at[side, at_chunk(k), :], plain_got.at[side, at_chunk(k), :], plain_sems, (side, k), {'data': peers[side]})
            plain[side, k].start()
    for k in range(SYNC_CHUNKS):
        for side in range(2):
            first[side, k].wait_recv()
            merged_send[side, at_chunk(k), :] = (first_got[side, at_chunk(k), :].astype(F32) + acc_in[rows_of(peers[side], side, k), :]).astype(BF16)
            merged[side, k] = remote(merged_send.at[side, at_chunk(k), :], merged_got.at[side, at_chunk(k), :], merged_sems, (side, k), {'data': peers[side]})
            merged[side, k].start()

    for copy in x_copies:
        copy.wait()
    total = rel_x[lax.rem(ent, groups)]
    for src in range(1, groups):
        total = total + rel_x[lax.rem(ent + groups - src, groups)]
    span = total.shape[0]
    rel_send_y[0:span, :] = total
    rel_send_y[span:, :] = loss_in[...]
    rel_y[0] = rel_send_y[...]
    y_copies = [remote(rel_send_y, rel_y.at[off], rel_y_sems, (off - 1,), {'data': lax.rem(me + off, reps)}) for off in range(1, reps)]
    for copy in y_copies:
        copy.start()

    own = {}
    for k in range(SYNC_CHUNKS):
        for which in range(2):
            merged[which, k].wait_recv()
            plain[1 - which, k].wait_recv()
            work[...] = acc_in[rows_of(me, which, k), :] + (merged_got[which, at_chunk(k), :].astype(F32) + plain_got[1 - which, at_chunk(k), :].astype(F32))
            n = chunk // 2
            re_g, im_g = work[pl.ds(0, n, stride=2), :], work[pl.ds(1, n, stride=2), :]
            places = pl.ds(which * (half // 2) + k * n, n)
            state = state_in[places, :] + jnp.sum(re_g * re_g + im_g * im_g, axis=1, keepdims=True) / width
            state_out[places, :] = state
            scale = learn_rate / jnp.sqrt(state + EPSILON)
            work[pl.ds(0, n, stride=2), :] = re_g * scale
            work[pl.ds(1, n, stride=2), :] = im_g * scale
            step_own[which, at_chunk(k), :] = work[...].astype(BF16)
            for side in range(2):
                own[side, which, k] = remote(step_own.at[which, at_chunk(k), :], step_got.at[side, which, at_chunk(k), :], own_sems, (side, which, k), {'data': peers[side]})
                own[side, which, k].start()

    spread = {}
    for k in range(SYNC_CHUNKS):
        for which in range(2):
            for side in range(2):
                own[side, which, k].wait_recv()
                if side == which:
                    spread[side, k] = remote(step_got.at[side, which, at_chunk(k), :], step_far.at[side, at_chunk(k), :], far_sems, (side, k), {'data': peers[side]})
                    spread[side, k].start()
            for owner, ref in ((me, step_own.at[which]), (peers[1], step_got.at[0, which]), (peers[0], step_got.at[1, which])):
                rows = rows_of(owner, which, k)
                table_out[rows, :] = table_in[rows, :] - ref[at_chunk(k), :].astype(F32)

    for copy in y_copies:
        copy.wait()
    total = rel_y[lax.rem(me, reps)]
    for src in range(1, reps):
        total = total + rel_y[lax.rem(me + reps - src, reps)]
    losses_out[...] = jnp.where(lax.broadcasted_iota(jnp.int32, losses_in.shape, 0) == shift, total[span:, :] / bucket_edges, losses_in[...])
    rel_send[...] = total[0:span, :]
    rel_rows = rel_send.shape[0] // 2
    re_g, im_g = rel_send[pl.ds(0, rel_rows, stride=2), :], rel_send[pl.ds(1, rel_rows, stride=2), :]
    state = rel_state_in[...] + jnp.sum(re_g * re_g + im_g * im_g, axis=1, keepdims=True) / width
    rel_state_out[...] = state
    scale = learn_rate / jnp.sqrt(state + EPSILON)
    rel_out[pl.ds(0, rel_rows, stride=2), :] = rel_in[pl.ds(0, rel_rows, stride=2), :] - re_g * scale
    rel_out[pl.ds(1, rel_rows, stride=2), :] = rel_in[pl.ds(1, rel_rows, stride=2), :] - im_g * scale

    state_copies = []
    if shift == groups - 1:
        eye = lax.broadcasted_iota(jnp.int32, (LANES, LANES), 0) == lax.broadcasted_iota(jnp.int32, (LANES, LANES), 1)
        blocks = state_own.shape[0]
        for at in range(blocks):
            state_own[at:at + 1, :] = jnp.sum(jnp.where(eye, state_out[at * LANES:(at + 1) * LANES, :], 0.0), axis=0, keepdims=True)
        place = pl.ds(pl.multiple_of(me * blocks, blocks), blocks)
        state_all[place, :] = state_own[...]
        state_copies = [remote(state_own, state_all.at[place, :], state_sems, (off - 1,), {'data': lax.rem(me + off, reps)}) for off in range(1, reps)]
        for copy in state_copies:
            copy.start()
    else:
        state_all[...] = jnp.zeros_like(state_all)

    for k in range(SYNC_CHUNKS):
        for side in range(2):
            spread[side, k].wait_recv()
            rows = rows_of(far, side, k)
            table_out[rows, :] = table_in[rows, :] - step_far[side, at_chunk(k), :].astype(F32)
    for group_of in (first, plain, merged, own, spread):
        for copy in group_of.values():
            copy.wait_send()
    for copy in state_copies:
        copy.wait()


def solution(mesh):
    groups = mesh.shape['ent']
    reps = mesh.shape['data']
    row_spec = P(('sweep', 'ent'), None)
    edge_spec = P(('sweep', 'ent'), None, 'data')
    vmem = pl.BlockSpec(memory_space=VM)

    def device_fn(ent_table, ent_state, rel_table, head_idx, tail_idx, rel_idx, edge_mask, neg_idx):
        part_rows, width = ent_table.shape
        rel_count = rel_table.shape[0]
        edges = head_idx.shape[2]
        negs = neg_idx.shape[2]
        bucket_edges = edges * reps
        learn_rate = LR_SCALE * width ** -0.25
        rel_pad = -(-rel_count // 8) * 8
        quarter = part_rows // reps
        me = lax.axis_index('data')

        packed = jnp.concatenate([tail_idx[0], edge_mask[0], neg_idx[0]], axis=1)
        moved = [packed[0:1]]
        for shift in range(1, groups):
            moved.append(lax.ppermute(packed[shift:shift + 1], 'ent', [(src, (src + shift) % groups) for src in range(groups)]))

        h_all = head_idx[0]
        r_all = rel_idx[0]
        row_grid = 8
        params = pltpu.CompilerParams(vmem_limit_bytes=VMEM_LIMIT)
        table = pl.pallas_call(
            functools.partial(load_kernel, width // 2), grid=(row_grid,),
            out_shape=jax.ShapeDtypeStruct((2 * part_rows, LANES), F32),
            in_specs=[pl.BlockSpec((width, part_rows // row_grid), lambda i: (0, i))],
            out_specs=pl.BlockSpec((2 * part_rows // row_grid, LANES), lambda i: (i, 0)),
            scratch_shapes=[VM((2 * LANES, part_rows // row_grid), F32)], name='load_table')(ent_table.T)
        rel = interleave(jnp.pad(rel_table, ((0, rel_pad - rel_count), (0, 0))))
        rel_state = jnp.zeros((rel_pad, LANES), F32)
        state = jnp.broadcast_to(lax.dynamic_slice_in_dim(ent_state, me * quarter, quarter)[:, None], (quarter, LANES))
        losses = jnp.zeros((-(-groups // 8) * 8, LANES), F32)

        smem = pl.BlockSpec(memory_space=pltpu.SMEM)
        sems = pltpu.SemaphoreType.DMA
        steps = edges // EDGE_BLOCK
        for shift in range(groups):
            tail = moved[shift]
            scratch = [VM((2 * edges, LANES), F32)] * 3 + [VM((2 * negs, LANES), F32), VM((edges, 2 * LANES), BF16),
                                                         VM((negs, 2 * LANES), BF16), VM((2 * LANES, negs), F32)]
            if shift:
                scratch += [VM((edges, 2 * LANES), BF16)] * 3 + [VM(losses.shape, F32), sems((2, steps)), sems((2, steps)), sems((2,))]
            else:
                scratch += [VM((edges, 2 * LANES), F32)]
            g_h, g_t, g_n, g_rel, loss = pl.pallas_call(
                functools.partial(bucket_kernel, shift, groups),
                out_shape=[jax.ShapeDtypeStruct((2 * edges, LANES), F32)] * 2
                + [jax.ShapeDtypeStruct((2 * negs, LANES), F32), jax.ShapeDtypeStruct((2 * rel_pad, LANES), F32), jax.ShapeDtypeStruct(losses.shape, F32)],
                in_specs=[smem] * 3 + [vmem] * 4, out_specs=[vmem] * 5, scratch_shapes=scratch,
                compiler_params=pltpu.CompilerParams(vmem_limit_bytes=VMEM_LIMIT, collective_id=0, has_side_effects=True) if shift else params,
                name='bucket',
            )(h_all, r_all, tail, table.reshape(part_rows, 2, LANES), rel.reshape(rel_pad, 2, LANES), r_all, tail)

            acc = pl.pallas_call(
                functools.partial(scatter_kernel, shift),
                out_shape=jax.ShapeDtypeStruct((2 * part_rows, LANES), F32),
                in_specs=[smem] * 2 + [vmem] * 3, out_specs=vmem,
                scratch_shapes=[VM((2 * part_rows, LANES), F32)] * 3,
                compiler_params=params, name='scatter_rows',
            )(h_all, tail, g_h, g_t, g_n)

            half = (2 * part_rows) // reps // 2
            block = VM((2, half, LANES), BF16)
            state_blocks = quarter // LANES
            table, state, rel, rel_state, losses, state_all = pl.pallas_call(
                functools.partial(update_kernel, width, learn_rate, groups, reps, shift, bucket_edges),
                out_shape=[jax.ShapeDtypeStruct(table.shape, F32), jax.ShapeDtypeStruct(state.shape, F32),
                           jax.ShapeDtypeStruct(rel.shape, F32), jax.ShapeDtypeStruct(rel_state.shape, F32),
                           jax.ShapeDtypeStruct(losses.shape, F32), jax.ShapeDtypeStruct((reps * state_blocks, LANES), F32)],
                in_specs=[vmem] * 8, out_specs=[vmem] * 6,
                scratch_shapes=[block] * 6 + [VM((half // SYNC_CHUNKS, LANES), F32), block, VM((2, 2, half, LANES), BF16), block,
                                              VM((groups, 2 * rel_pad, LANES), F32), VM((reps, 2 * rel_pad + losses.shape[0], LANES), F32), VM((2 * rel_pad, LANES), F32),
                                              VM((2 * rel_pad + losses.shape[0], LANES), F32), VM((state_blocks, LANES), F32),
                                              sems((2, 2, SYNC_CHUNKS)), sems((2, 2, SYNC_CHUNKS)), sems((2, 2, SYNC_CHUNKS)),
                                              sems((2, 2, 2, SYNC_CHUNKS)), sems((2, 2, SYNC_CHUNKS)), sems((2, groups - 1)), sems((2, reps - 1)), sems((2, reps - 1))],
                compiler_params=pltpu.CompilerParams(vmem_limit_bytes=VMEM_LIMIT, collective_id=1, has_side_effects=True), name='update',
            )(acc, table, state, g_rel, rel, rel_state, loss, losses)

        ent_out = pl.pallas_call(
            functools.partial(store_kernel, width // 2), grid=(row_grid,),
            out_shape=jax.ShapeDtypeStruct((width, part_rows), F32),
            in_specs=[pl.BlockSpec((2 * part_rows // row_grid, LANES), lambda i: (i, 0))],
            out_specs=pl.BlockSpec((width, part_rows // row_grid), lambda i: (0, i)), name='store_table')(table).T
        rel_out = deinterleave(rel, width)[:rel_count]
        return ent_out, state_all.reshape(part_rows), rel_out, losses[:groups, 0].reshape(1, groups)

    return jax.shard_map(device_fn, mesh=mesh, in_specs=(row_spec, P(('sweep', 'ent')), P('sweep', None), edge_spec, edge_spec, edge_spec, edge_spec, P(('sweep', 'ent'), None, None)), out_specs=(row_spec, P(('sweep', 'ent')), P('sweep', None), row_spec), check_vma=False)
```

```python
import functools

import jax
import jax.numpy as jnp
from jax import lax
from jax.experimental import pallas as pl
from jax.experimental.pallas import tpu as pltpu
from jax.sharding import PartitionSpec as P

LR_SCALE = 0.2
EPSILON = 1e-8
LANES = 128
EDGE_BLOCK = 256
GATHER_UNROLL = 16
SYNC_CHUNKS = 4
VMEM_LIMIT = 60 * 1024 * 1024
MESH = pl.DeviceIdType.MESH
VM = pltpu.VMEM
F32 = jnp.float32
BF16 = jnp.bfloat16


def interleave(table):
    rows, width = table.shape
    half = width // 2
    return jnp.pad(table.reshape(rows, 2, half), ((0, 0), (0, 0), (0, LANES - half))).reshape(rows * 2, LANES)


def deinterleave(table, width):
    rows = table.shape[0] // 2
    return table.reshape(rows, 2, LANES)[:, :, :width // 2].reshape(rows, width)


def pair(row):
    return pl.ds(pl.multiple_of(row * 2, 2), 2)


def load_kernel(half, table_t, table, staged):
    width, cols = table_t.shape
    staged[0:width, :] = table_t[...]
    staged[width:2 * LANES, :] = jnp.zeros((2 * LANES - width, cols), F32)
    lane = lax.broadcasted_iota(jnp.int32, (LANES, LANES), 1)
    for at in range(0, cols, LANES):
        low = staged[0:LANES, at:at + LANES].T
        high = staged[LANES:2 * LANES, at:at + LANES].T
        table[pl.ds(2 * at, LANES, stride=2), :] = jnp.where(lane < half, low, 0.0)
        moved = jnp.where(lane < LANES - half, pltpu.roll(low, LANES - half, 1), pltpu.roll(high, LANES - half, 1))
        table[pl.ds(2 * at + 1, LANES, stride=2), :] = jnp.where(lane < half, moved, 0.0)


def store_kernel(half, table, table_t):
    width, cols = table_t.shape
    lane = lax.broadcasted_iota(jnp.int32, (LANES, LANES), 1)
    for at in range(0, cols, LANES):
        re = table[pl.ds(2 * at, LANES, stride=2), :]
        moved = pltpu.roll(table[pl.ds(2 * at + 1, LANES, stride=2), :], half, 1)
        table_t[0:LANES, at:at + LANES] = jnp.where(lane < half, re, moved).T
        table_t[LANES:width, at:at + LANES] = moved.T[0:width - LANES, :]


def bucket_kernel(shift, group, h_ids, r_ids, tail_ids, table, rel, r_vec, tail_vec,
                  gh_ref, gt_ref, gn_ref, grel_ref, loss_ref,
                  h_rows, r_rows, t_rows, n_rows, q_own, n_bf, gn_acc, *scratch):
    edges = q_own.shape[0]
    negs = n_bf.shape[0]
    rel_pad = grel_ref.shape[0] // 2
    steps = edges // EDGE_BLOCK

    def block(step):
        return pl.ds(pl.multiple_of(step * EDGE_BLOCK, EDGE_BLOCK), EDGE_BLOCK)

    def halves(base, count):
        return pl.ds(pl.multiple_of(2 * base, 2), count, stride=2), pl.ds(2 * base + 1, count, stride=2)

    if shift:
        q_got, gq_send, gq_got, loss_send, q_sems, gq_sems, loss_sems = scratch
        me = lax.axis_index('ent')
        ahead = lax.rem(me + shift, group)
        behind = lax.rem(me + group - shift, group)

        def q_copy(step):
            return pltpu.make_async_remote_copy(
                src_ref=q_own.at[block(step), :], dst_ref=q_got.at[block(step), :],
                send_sem=q_sems.at[0, step], recv_sem=q_sems.at[1, step],
                device_id={'ent': ahead}, device_id_type=MESH)

        def gq_copy(step):
            return pltpu.make_async_remote_copy(
                src_ref=gq_send.at[block(step), :], dst_ref=gq_got.at[block(step), :],
                send_sem=gq_sems.at[0, step], recv_sem=gq_sems.at[1, step],
                device_id={'ent': behind}, device_id_type=MESH)

        barrier = pltpu.get_barrier_semaphore()
        pl.semaphore_signal(barrier, inc=1, device_id={'ent': ahead}, device_id_type=MESH)
        pl.semaphore_signal(barrier, inc=1, device_id={'ent': behind}, device_id_type=MESH)
        pl.semaphore_wait(barrier, 2)
        q_src, gq_src, gq_dst = q_got, gq_got, gq_send
    else:
        gq_got, = scratch
        q_src, gq_src, gq_dst = q_own, gq_got, gq_got

    def ask(step, _):
        def gather(part, _):
            base = step * EDGE_BLOCK + part * GATHER_UNROLL
            for off in range(GATHER_UNROLL):
                at = base + off
                h_rows[pair(at), :] = table[h_ids[shift, at]]
                r_rows[pair(at), :] = rel[r_ids[shift, at]]
            return 0

        lax.fori_loop(0, EDGE_BLOCK // GATHER_UNROLL, gather, 0)
        rows = block(step)
        even, odd = halves(step * EDGE_BLOCK, EDGE_BLOCK)
        re_h, im_h = h_rows[even, :], h_rows[odd, :]
        re_r, im_r = r_rows[even, :], r_rows[odd, :]
        q_own[rows, 0:LANES] = (re_h * re_r - im_h * im_r).astype(BF16)
        q_own[rows, LANES:2 * LANES] = (re_h * im_r + im_h * re_r).astype(BF16)
        if shift:
            q_copy(step).start()
        return 0

    lax.fori_loop(0, steps, ask, 0)

    def gather_negs(part, _):
        for off in range(GATHER_UNROLL):
            at = part * GATHER_UNROLL + off
            n_rows[pair(at), :] = table[tail_ids[0, 2 * edges + at]]
        return 0

    lax.fori_loop(0, negs // GATHER_UNROLL, gather_negs, 0)
    n_even, n_odd = halves(0, negs)
    n_bf[:, 0:LANES] = n_rows[n_even, :].astype(BF16)
    n_bf[:, LANES:2 * LANES] = n_rows[n_odd, :].astype(BF16)

    def gather_tails(part, _):
        for off in range(GATHER_UNROLL):
            at = part * GATHER_UNROLL + off
            t_rows[pair(at), :] = table[tail_ids[0, at]]
        return 0

    lax.fori_loop(0, edges // GATHER_UNROLL, gather_tails, 0)

    gn_acc[...] = jnp.zeros_like(gn_acc)
    eye = lax.broadcasted_iota(jnp.int32, (LANES, LANES), 0) == lax.broadcasted_iota(jnp.int32, (LANES, LANES), 1)
    per_block = EDGE_BLOCK // LANES

    def answer(step, loss_acc):
        if shift:
            q_copy(step).wait_recv()
        rows = block(step)
        even, odd = halves(step * EDGE_BLOCK, EDGE_BLOCK)
        q = q_src[rows, :]
        t = jnp.concatenate([t_rows[even, :].astype(BF16), t_rows[odd, :].astype(BF16)], axis=1).astype(F32)
        q_wide = q.astype(F32)
        n = n_bf[...]
        masks = [tail_vec[0:1, pl.ds(pl.multiple_of(edges + step * EDGE_BLOCK + k * LANES, LANES), LANES)].astype(F32) for k in range(per_block)]
        w = jnp.concatenate([jnp.sum(jnp.where(eye, mask, 0.0), axis=1, keepdims=True) for mask in masks], axis=0)
        pos = jnp.sum(q_wide * t, axis=1, keepdims=True)
        score = lax.dot_general(q, n, (((1,), (1,)), ((), ())), preferred_element_type=F32)
        top = jnp.maximum(jnp.max(score, axis=1, keepdims=True), pos)
        pos_exp = jnp.exp(pos - top)
        neg_exp = jnp.exp(score - top)
        total = pos_exp + jnp.sum(neg_exp, axis=1, keepdims=True)
        loss_acc = loss_acc + jnp.sum(w * (top + jnp.log(total) - pos), axis=0, keepdims=True)
        d_pos = w * (pos_exp / total - 1.0)
        d_neg = ((w / total) * neg_exp).astype(BF16)
        gq_dst[rows, :] = (d_pos * t + jnp.dot(d_neg, n, preferred_element_type=F32)).astype(gq_dst.dtype)
        g_tail = d_pos * q_wide
        gt_ref[even, :] = g_tail[:, 0:LANES]
        gt_ref[odd, :] = g_tail[:, LANES:2 * LANES]
        gn_acc[...] += lax.dot_general(q, d_neg, (((0,), (0,)), ((), ())), preferred_element_type=F32)
        if shift:
            gq_copy(step).start()
        return loss_acc

    loss = lax.fori_loop(0, steps, answer, jnp.zeros((1, 1), F32))
    if shift:
        loss_send[...] = jnp.broadcast_to(loss, loss_send.shape)
        loss_copy = pltpu.make_async_remote_copy(
            src_ref=loss_send, dst_ref=loss_ref, send_sem=loss_sems.at[0], recv_sem=loss_sems.at[1],
            device_id={'ent': behind}, device_id_type=MESH)
        loss_copy.start()
    else:
        loss_ref[...] = jnp.broadcast_to(loss, loss_ref.shape)
    for half in range(2):
        gn_ref[pl.ds(half, negs, stride=2), :] = gn_acc[half * LANES:(half + 1) * LANES, :].T

    def finish(step, carry):
        rel_re, rel_im = carry
        if shift:
            gq_copy(step).wait_recv()
        rows = block(step)
        even, odd = halves(step * EDGE_BLOCK, EDGE_BLOCK)
        re_g, im_g = gq_src[rows, 0:LANES].astype(F32), gq_src[rows, LANES:2 * LANES].astype(F32)
        re_r, im_r = r_rows[even, :], r_rows[odd, :]
        gh_ref[even, :] = re_g * re_r + im_g * im_r
        gh_ref[odd, :] = im_g * re_r - re_g * im_r
        re_h, im_h = h_rows[even, :], h_rows[odd, :]
        ids = r_vec[shift:shift + 1, pl.ds(pl.multiple_of(step * EDGE_BLOCK, EDGE_BLOCK), EDGE_BLOCK)]
        hot = (lax.broadcasted_iota(jnp.int32, (rel_pad, EDGE_BLOCK), 0) == ids).astype(F32)
        rel_re = rel_re + jnp.dot(hot, re_g * re_h + im_g * im_h, precision=lax.Precision.HIGHEST, preferred_element_type=F32)
        rel_im = rel_im + jnp.dot(hot, im_g * re_h - re_g * im_h, precision=lax.Precision.HIGHEST, preferred_element_type=F32)
        return rel_re, rel_im

    zero = jnp.zeros((rel_pad, LANES), F32)
    rel_re, rel_im = lax.fori_loop(0, steps, finish, (zero, zero))
    grel_ref[pl.ds(0, rel_pad, stride=2), :] = rel_re
    grel_ref[pl.ds(1, rel_pad, stride=2), :] = rel_im
    if shift:
        loss_copy.wait()

        def drain(step, _):
            q_copy(step).wait_send()
            gq_copy(step).wait_send()
            return 0

        lax.fori_loop(0, steps, drain, 0)


def scatter_kernel(shift, h_ids, tail_ids, gh_in, gt_in, gn_in, acc_out, acc, acc_b, acc_c, acc_d, gh, gt_ref, gn_ref, in_sems, out_sems):
    edges = gh.shape[0] // 2
    negs = gn_ref.shape[0] // 2
    table_rows = acc.shape[0]
    zero_rows = 512
    pieces = 8
    piece = table_rows // pieces

    copies = [pltpu.make_async_copy(src, dst, in_sems.at[at]) for at, (src, dst) in enumerate(((gh_in, gh), (gt_in, gt_ref), (gn_in, gn_ref)))]
    for copy in copies:
        copy.start()

    def clear(step, _):
        rows = pl.ds(pl.multiple_of(step * zero_rows, zero_rows), zero_rows)
        for ref in (acc, acc_b, acc_c, acc_d):
            ref[rows, :] = jnp.zeros((zero_rows, LANES), F32)
        return 0

    lax.fori_loop(0, table_rows // zero_rows, clear, 0)
    for copy in copies:
        copy.wait()

    def add_edges(step, _):
        base = step * GATHER_UNROLL
        for off in range(0, GATHER_UNROLL, 2):
            at = base + off
            places = (pair(h_ids[shift, at]), pair(h_ids[shift, at + 1]), pair(tail_ids[0, at]), pair(tail_ids[0, at + 1]))
            refs = (acc, acc_b, acc_c, acc_d)
            terms = (gh[pair(at), :], gh[pair(at + 1), :], gt_ref[pair(at), :], gt_ref[pair(at + 1), :])
            sums = [ref[place, :] + term for ref, place, term in zip(refs, places, terms)]
            for ref, place, total in zip(refs, places, sums):
                ref[place, :] = total
        return 0

    lax.fori_loop(0, edges // GATHER_UNROLL, add_edges, 0)

    def add_negs(step, _):
        base = step * GATHER_UNROLL
        for off in range(0, GATHER_UNROLL, 4):
            at = base + off
            places = [pair(tail_ids[0, 2 * edges + at + k]) for k in range(4)]
            refs = (acc, acc_b, acc_c, acc_d)
            sums = [ref[place, :] + gn_ref[pair(at + k), :] for k, (ref, place) in enumerate(zip(refs, places))]
            for ref, place, total in zip(refs, places, sums):
                ref[place, :] = total
        return 0

    lax.fori_loop(0, negs // GATHER_UNROLL, add_negs, 0)

    def out_copy(at):
        rows = pl.ds(pl.multiple_of(at * piece, piece), piece)
        return pltpu.make_async_copy(acc.at[rows, :], acc_out.at[rows, :], out_sems.at[at])

    def combine(at, _):
        rows = pl.ds(pl.multiple_of(at * piece, piece), piece)
        acc[rows, :] = (acc[rows, :] + acc_b[rows, :]) + (acc_c[rows, :] + acc_d[rows, :])
        out_copy(at).start()
        return 0

    lax.fori_loop(0, pieces, combine, 0)
    for at in range(pieces):
        out_copy(at).wait()


def pieces_of(half):
    found, at = [], 0
    for bit in range(7, -1, -1):
        if half >> bit & 1:
            found.append((1 << bit, at))
            at += 1 << bit
    return found


def pack_rows(half, x):
    n = x.shape[0]
    lane = lax.broadcasted_iota(jnp.int32, (1, LANES), 1)
    out = []
    for size, at in pieces_of(half):
        groups = LANES // size
        rows = n // groups
        acc = None
        for k in range(groups):
            part = pltpu.roll(x[k * rows:(k + 1) * rows], (k * size - at) % LANES, 1)
            acc = part if acc is None else jnp.where(lane < k * size, acc, part)
        out.append(acc)
    return jnp.concatenate(out, axis=0)


def unpack_rows(half, n, x):
    lane = lax.broadcasted_iota(jnp.int32, (1, LANES), 1)
    out, start = None, 0
    for size, at in pieces_of(half):
        groups = LANES // size
        rows = n // groups
        block = x[start:start + rows]
        start += rows
        parts = jnp.concatenate([pltpu.roll(block, (at - k * size) % LANES, 1) for k in range(groups)], axis=0)
        out = parts if out is None else jnp.where(lane < at, out, parts)
    return jnp.where(lane < half, out, 0.0)


def update_kernel(width, learn_rate, groups, reps, shift, bucket_edges, acc_hbm, table_hbm, state_in, grel_in, rel_in, rel_state_in, loss_in, losses_in,
                  table_out, state_out, rel_out, rel_state_out, losses_out, state_all,
                  acc, table, first_send, first_got, plain_send, plain_got, merged_send, merged_got, work,
                  step_own, step_got, step_far, rel_x, rel_y, rel_send, rel_send_y, state_own, acc_sems, table_sems, out_sems,
                  first_sems, plain_sems, merged_sems, own_sems, far_sems, rel_x_sems, rel_y_sems, state_sems):
    me = lax.axis_index('data')
    ent = lax.axis_index('ent')
    used = width // 2
    peers = (lax.rem(me + 1, reps), lax.rem(me + reps - 1, reps))
    peer_slots = (1, reps - 1)
    half = acc.shape[2]
    chunk = half // SYNC_CHUNKS
    sent = chunk * used // LANES

    def part_rows(slot, which):
        return pl.ds(pl.multiple_of((lax.rem(me + slot, reps) * 2 + which) * half, half), half)

    def load(src, dst, sems, slot, which):
        return pltpu.make_async_copy(src.at[part_rows(slot, which), :], dst.at[slot, which], sems.at[slot, which])

    def save(slot, which):
        return pltpu.make_async_copy(table.at[slot, which], table_out.at[part_rows(slot, which), :], out_sems.at[slot, which])

    for slot, which in ((2, 0), (2, 1), (1, 1), (3, 0), (1, 0), (3, 1), (0, 0), (0, 1)):
        load(acc_hbm, acc, acc_sems, slot, which).start()
    for slot in range(reps):
        for which in range(2):
            load(table_hbm, table, table_sems, slot, which).start()

    barrier = pltpu.get_barrier_semaphore()
    for off in range(1, reps):
        pl.semaphore_signal(barrier, inc=1, device_id={'data': lax.rem(me + off, reps)}, device_id_type=MESH)
    for off in range(1, groups):
        pl.semaphore_signal(barrier, inc=1, device_id={'ent': lax.rem(ent + off, groups)}, device_id_type=MESH)
    pl.semaphore_wait(barrier, reps + groups - 2)

    def remote(src, dst, sems, place, to):
        return pltpu.make_async_remote_copy(
            src_ref=src, dst_ref=dst, send_sem=sems.at[(0,) + place], recv_sem=sems.at[(1,) + place],
            device_id=to, device_id_type=MESH)

    rel_x[0] = grel_in[...]
    rel_send[...] = grel_in[...]
    x_copies = [remote(rel_send, rel_x.at[off], rel_x_sems, (off - 1,), {'ent': lax.rem(ent + off, groups)}) for off in range(1, groups)]
    for copy in x_copies:
        copy.start()

    def at_chunk(k):
        return pl.ds(pl.multiple_of(k * chunk, chunk), chunk)

    def at_sent(k):
        return pl.ds(pl.multiple_of(k * sent, sent), sent)

    def first(side, k):
        return remote(first_send.at[side, at_sent(k), :], first_got.at[side, at_sent(k), :], first_sems, (side, k), {'data': peers[side]})

    def plain(side, k):
        return remote(plain_send.at[side, at_sent(k), :], plain_got.at[side, at_sent(k), :], plain_sems, (side, k), {'data': peers[side]})

    def merged(side, k):
        return remote(merged_send.at[side, at_sent(k), :], merged_got.at[side, at_sent(k), :], merged_sems, (side, k), {'data': peers[side]})

    def own(side, which, k):
        return remote(step_own.at[which, at_sent(k), :], step_got.at[side, which, at_sent(k), :], own_sems, (side, which, k), {'data': peers[side]})

    def spread(side, k):
        return remote(step_got.at[side, side, at_sent(k), :], step_far.at[side, at_sent(k), :], far_sems, (side, k), {'data': peers[side]})

    def send_first(k, _):
        for side in range(2):
            first_send[side, at_sent(k), :] = pack_rows(used, acc[2, side, at_chunk(k), :]).astype(BF16)
            first(side, k).start()
        return 0

    def send_plain(k, _):
        for side in range(2):
            plain_send[side, at_sent(k), :] = pack_rows(used, acc[peer_slots[side], 1 - side, at_chunk(k), :]).astype(BF16)
            plain(side, k).start()
        return 0

    def send_merged(k, _):
        for side in range(2):
            first(side, k).wait_recv()
            merged_send[side, at_sent(k), :] = (first_got[side, at_sent(k), :].astype(F32) + pack_rows(used, acc[peer_slots[side], side, at_chunk(k), :])).astype(BF16)
            merged(side, k).start()
        return 0

    for needed, body in ((((2, 0), (2, 1)), send_first), (((1, 1), (3, 0)), send_plain), (((1, 0), (3, 1)), send_merged)):
        for slot, which in needed:
            load(acc_hbm, acc, acc_sems, slot, which).wait()
        lax.fori_loop(0, SYNC_CHUNKS, body, 0)

    for copy in x_copies:
        copy.wait()
    total = rel_x[lax.rem(ent, groups)]
    for src in range(1, groups):
        total = total + rel_x[lax.rem(ent + groups - src, groups)]
    span = total.shape[0]
    rel_send_y[0:span, :] = total
    rel_send_y[span:, :] = loss_in[...]
    rel_y[0] = rel_send_y[...]
    y_copies = [remote(rel_send_y, rel_y.at[off], rel_y_sems, (off - 1,), {'data': lax.rem(me + off, reps)}) for off in range(1, reps)]
    for copy in y_copies:
        copy.start()

    for which in range(2):
        load(acc_hbm, acc, acc_sems, 0, which).wait()
    for slot in range(reps):
        for which in range(2):
            load(table_hbm, table, table_sems, slot, which).wait()
    n = chunk // 2
    even, odd = pl.ds(0, n, stride=2), pl.ds(1, n, stride=2)

    def step_rows(k, _):
        for which in range(2):
            merged(which, k).wait_recv()
            plain(1 - which, k).wait_recv()
            others = merged_got[which, at_sent(k), :].astype(F32) + plain_got[1 - which, at_sent(k), :].astype(F32)
            work[...] = acc[0, which, at_chunk(k), :] + unpack_rows(used, chunk, others)
            re_g, im_g = work[even, :], work[odd, :]
            places = pl.ds(pl.multiple_of(which * (half // 2) + k * n, n), n)
            state = state_in[places, :] + jnp.sum(re_g * re_g + im_g * im_g, axis=1, keepdims=True) / width
            state_out[places, :] = state
            scale = learn_rate / jnp.sqrt(state + EPSILON)
            work[even, :] = re_g * scale
            work[odd, :] = im_g * scale
            moves = work[...]
            step_own[which, at_sent(k), :] = pack_rows(used, moves).astype(BF16)
            for side in range(2):
                own(side, which, k).start()
            table[0, which, at_chunk(k), :] -= moves.astype(BF16).astype(F32)
        return 0

    lax.fori_loop(0, SYNC_CHUNKS, step_rows, 0)
    for which in range(2):
        save(0, which).start()

    def take_near(k, _):
        for which in range(2):
            for side in (which, 1 - which):
                own(side, which, k).wait_recv()
                if side == which:
                    spread(side, k).start()
                table[peer_slots[1 - side], which, at_chunk(k), :] -= unpack_rows(used, chunk, step_got[side, which, at_sent(k), :].astype(F32))
        return 0

    lax.fori_loop(0, SYNC_CHUNKS, take_near, 0)
    for slot in peer_slots:
        for which in range(2):
            save(slot, which).start()

    for copy in y_copies:
        copy.wait()
    total = rel_y[lax.rem(me, reps)]
    for src in range(1, reps):
        total = total + rel_y[lax.rem(me + reps - src, reps)]
    losses_out[...] = jnp.where(lax.broadcasted_iota(jnp.int32, losses_in.shape, 0) == shift, total[span:, :] / bucket_edges, losses_in[...])
    rel_send[...] = total[0:span, :]
    rel_rows = rel_send.shape[0] // 2
    re_g, im_g = rel_send[pl.ds(0, rel_rows, stride=2), :], rel_send[pl.ds(1, rel_rows, stride=2), :]
    state = rel_state_in[...] + jnp.sum(re_g * re_g + im_g * im_g, axis=1, keepdims=True) / width
    rel_state_out[...] = state
    scale = learn_rate / jnp.sqrt(state + EPSILON)
    rel_out[pl.ds(0, rel_rows, stride=2), :] = rel_in[pl.ds(0, rel_rows, stride=2), :] - re_g * scale
    rel_out[pl.ds(1, rel_rows, stride=2), :] = rel_in[pl.ds(1, rel_rows, stride=2), :] - im_g * scale

    state_copies = []
    if shift == groups - 1:
        eye = lax.broadcasted_iota(jnp.int32, (LANES, LANES), 0) == lax.broadcasted_iota(jnp.int32, (LANES, LANES), 1)
        blocks = state_own.shape[0]
        for at in range(blocks):
            state_own[at:at + 1, :] = jnp.sum(jnp.where(eye, state_out[at * LANES:(at + 1) * LANES, :], 0.0), axis=0, keepdims=True)
        place = pl.ds(pl.multiple_of(me * blocks, blocks), blocks)
        state_all[place, :] = state_own[...]
        state_copies = [remote(state_own, state_all.at[place, :], state_sems, (off - 1,), {'data': lax.rem(me + off, reps)}) for off in range(1, reps)]
        for copy in state_copies:
            copy.start()
    else:
        state_all[...] = jnp.zeros_like(state_all)

    def take_far(k, _):
        for side in range(2):
            spread(side, k).wait_recv()
            table[2, side, at_chunk(k), :] -= unpack_rows(used, chunk, step_far[side, at_sent(k), :].astype(F32))
        return 0

    lax.fori_loop(0, SYNC_CHUNKS, take_far, 0)
    for which in range(2):
        save(2, which).start()

    def drain(k, _):
        for side in range(2):
            for copy in (first(side, k), plain(side, k), merged(side, k), own(side, 0, k), own(side, 1, k), spread(side, k)):
                copy.wait_send()
        return 0

    lax.fori_loop(0, SYNC_CHUNKS, drain, 0)
    for slot in range(reps):
        for which in range(2):
            save(slot, which).wait()
    for copy in state_copies:
        copy.wait()


def solution(mesh):
    groups = mesh.shape['ent']
    reps = mesh.shape['data']
    row_spec = P(('sweep', 'ent'), None)
    edge_spec = P(('sweep', 'ent'), None, 'data')
    vmem = pl.BlockSpec(memory_space=VM)

    def device_fn(ent_table, ent_state, rel_table, head_idx, tail_idx, rel_idx, edge_mask, neg_idx):
        part_rows, width = ent_table.shape
        rel_count = rel_table.shape[0]
        edges = head_idx.shape[2]
        negs = neg_idx.shape[2]
        bucket_edges = edges * reps
        learn_rate = LR_SCALE * width ** -0.25
        rel_pad = -(-rel_count // 8) * 8
        quarter = part_rows // reps
        me = lax.axis_index('data')

        packed = jnp.concatenate([tail_idx[0], edge_mask[0], neg_idx[0]], axis=1)
        moved = [packed[0:1]]
        for shift in range(1, groups):
            moved.append(lax.ppermute(packed[shift:shift + 1], 'ent', [(src, (src + shift) % groups) for src in range(groups)]))

        h_all = head_idx[0]
        r_all = rel_idx[0]
        row_grid = 8
        params = pltpu.CompilerParams(vmem_limit_bytes=VMEM_LIMIT)
        table = pl.pallas_call(
            functools.partial(load_kernel, width // 2), grid=(row_grid,),
            out_shape=jax.ShapeDtypeStruct((2 * part_rows, LANES), F32),
            in_specs=[pl.BlockSpec((width, part_rows // row_grid), lambda i: (0, i))],
            out_specs=pl.BlockSpec((2 * part_rows // row_grid, LANES), lambda i: (i, 0)),
            scratch_shapes=[VM((2 * LANES, part_rows // row_grid), F32)], name='load_table')(ent_table.T)
        rel = interleave(jnp.pad(rel_table, ((0, rel_pad - rel_count), (0, 0))))
        rel_state = jnp.zeros((rel_pad, LANES), F32)
        state = jnp.broadcast_to(lax.dynamic_slice_in_dim(ent_state, me * quarter, quarter)[:, None], (quarter, LANES))
        losses = jnp.zeros((-(-groups // 8) * 8, LANES), F32)

        smem = pl.BlockSpec(memory_space=pltpu.SMEM)
        hbm = pl.BlockSpec(memory_space=pl.ANY)
        sems = pltpu.SemaphoreType.DMA
        steps = edges // EDGE_BLOCK
        for shift in range(groups):
            tail = moved[shift]
            scratch = [VM((2 * edges, LANES), F32)] * 3 + [VM((2 * negs, LANES), F32), VM((edges, 2 * LANES), BF16),
                                                         VM((negs, 2 * LANES), BF16), VM((2 * LANES, negs), F32)]
            if shift:
                scratch += [VM((edges, 2 * LANES), BF16)] * 3 + [VM(losses.shape, F32), sems((2, steps)), sems((2, steps)), sems((2,))]
            else:
                scratch += [VM((edges, 2 * LANES), F32)]
            g_h, g_t, g_n, g_rel, loss = pl.pallas_call(
                functools.partial(bucket_kernel, shift, groups),
                out_shape=[jax.ShapeDtypeStruct((2 * edges, LANES), F32)] * 2
                + [jax.ShapeDtypeStruct((2 * negs, LANES), F32), jax.ShapeDtypeStruct((2 * rel_pad, LANES), F32), jax.ShapeDtypeStruct(losses.shape, F32)],
                in_specs=[smem] * 3 + [vmem] * 4, out_specs=[vmem] * 5, scratch_shapes=scratch,
                compiler_params=pltpu.CompilerParams(vmem_limit_bytes=VMEM_LIMIT, collective_id=0, has_side_effects=True) if shift else params,
                name='bucket',
            )(h_all, r_all, tail, table.reshape(part_rows, 2, LANES), rel.reshape(rel_pad, 2, LANES), r_all, tail)

            acc = pl.pallas_call(
                functools.partial(scatter_kernel, shift),
                out_shape=jax.ShapeDtypeStruct((2 * part_rows, LANES), F32),
                in_specs=[smem] * 2 + [hbm] * 3, out_specs=hbm,
                scratch_shapes=[VM((2 * part_rows, LANES), F32)] * 4 + [VM((2 * edges, LANES), F32)] * 2 + [VM((2 * negs, LANES), F32), sems((3,)), sems((8,))],
                compiler_params=params, name='scatter_rows',
            )(h_all, tail, g_h, g_t, g_n)

            half = (2 * part_rows) // reps // 2
            half_sent = half * (width // 2) // LANES
            block = VM((2, half_sent, LANES), BF16)
            state_blocks = quarter // LANES
            table, state, rel, rel_state, losses, state_all = pl.pallas_call(
                functools.partial(update_kernel, width, learn_rate, groups, reps, shift, bucket_edges),
                out_shape=[jax.ShapeDtypeStruct(table.shape, F32), jax.ShapeDtypeStruct(state.shape, F32),
                           jax.ShapeDtypeStruct(rel.shape, F32), jax.ShapeDtypeStruct(rel_state.shape, F32),
                           jax.ShapeDtypeStruct(losses.shape, F32), jax.ShapeDtypeStruct((reps * state_blocks, LANES), F32)],
                in_specs=[hbm] * 2 + [vmem] * 6, out_specs=[hbm] + [vmem] * 5,
                scratch_shapes=[VM((reps, 2, half, LANES), F32)] * 2 + [block] * 6 + [VM((half // SYNC_CHUNKS, LANES), F32), block, VM((2, 2, half_sent, LANES), BF16), block,
                                              VM((groups, 2 * rel_pad, LANES), F32), VM((reps, 2 * rel_pad + losses.shape[0], LANES), F32), VM((2 * rel_pad, LANES), F32),
                                              VM((2 * rel_pad + losses.shape[0], LANES), F32), VM((state_blocks, LANES), F32), sems((reps, 2)), sems((reps, 2)), sems((reps, 2)),
                                              sems((2, 2, SYNC_CHUNKS)), sems((2, 2, SYNC_CHUNKS)), sems((2, 2, SYNC_CHUNKS)),
                                              sems((2, 2, 2, SYNC_CHUNKS)), sems((2, 2, SYNC_CHUNKS)), sems((2, groups - 1)), sems((2, reps - 1)), sems((2, reps - 1))],
                compiler_params=pltpu.CompilerParams(vmem_limit_bytes=VMEM_LIMIT, collective_id=1, has_side_effects=True), name='update',
            )(acc, table, state, g_rel, rel, rel_state, loss, losses)

        ent_out = pl.pallas_call(
            functools.partial(store_kernel, width // 2), grid=(row_grid,),
            out_shape=jax.ShapeDtypeStruct((width, part_rows), F32),
            in_specs=[pl.BlockSpec((2 * part_rows // row_grid, LANES), lambda i: (i, 0))],
            out_specs=pl.BlockSpec((width, part_rows // row_grid), lambda i: (0, i)), name='store_table')(table).T
        rel_out = deinterleave(rel, width)[:rel_count]
        return ent_out, state_all.reshape(part_rows), rel_out, losses[:groups, 0].reshape(1, groups)

    return jax.shard_map(device_fn, mesh=mesh, in_specs=(row_spec, P(('sweep', 'ent')), P('sweep', None), edge_spec, edge_spec, edge_spec, edge_spec, P(('sweep', 'ent'), None, None)), out_specs=(row_spec, P(('sweep', 'ent')), P('sweep', None), row_spec), check_vma=False)
```

```python
import functools

import jax
import jax.numpy as jnp
from jax import lax
from jax.experimental import pallas as pl
from jax.experimental.pallas import tpu as pltpu
from jax.sharding import PartitionSpec as P

LR_SCALE = 0.2
EPSILON = 1e-8
LANES = 128
EDGE_BLOCK = 256
GATHER_UNROLL = 32
SCATTER_UNROLL = 16
SYNC_CHUNKS = 4
VMEM_LIMIT = 60 * 1024 * 1024
MESH = pl.DeviceIdType.MESH
VM = pltpu.VMEM
F32 = jnp.float32
BF16 = jnp.bfloat16


def interleave(table):
    rows, width = table.shape
    half = width // 2
    return jnp.pad(table.reshape(rows, 2, half), ((0, 0), (0, 0), (0, LANES - half))).reshape(rows * 2, LANES)


def deinterleave(table, width):
    rows = table.shape[0] // 2
    return table.reshape(rows, 2, LANES)[:, :, :width // 2].reshape(rows, width)


def pair(row):
    return pl.ds(pl.multiple_of(row * 2, 2), 2)


def load_kernel(half, table_t, table, staged):
    width, cols = table_t.shape
    staged[0:width, :] = table_t[...]
    staged[width:2 * LANES, :] = jnp.zeros((2 * LANES - width, cols), F32)
    lane = lax.broadcasted_iota(jnp.int32, (LANES, LANES), 1)
    for at in range(0, cols, LANES):
        low = staged[0:LANES, at:at + LANES].T
        high = staged[LANES:2 * LANES, at:at + LANES].T
        table[pl.ds(2 * at, LANES, stride=2), :] = jnp.where(lane < half, low, 0.0)
        moved = jnp.where(lane < LANES - half, pltpu.roll(low, LANES - half, 1), pltpu.roll(high, LANES - half, 1))
        table[pl.ds(2 * at + 1, LANES, stride=2), :] = jnp.where(lane < half, moved, 0.0)


def store_kernel(half, table, table_t):
    width, cols = table_t.shape
    lane = lax.broadcasted_iota(jnp.int32, (LANES, LANES), 1)
    for at in range(0, cols, LANES):
        re = table[pl.ds(2 * at, LANES, stride=2), :]
        moved = pltpu.roll(table[pl.ds(2 * at + 1, LANES, stride=2), :], half, 1)
        table_t[0:LANES, at:at + LANES] = jnp.where(lane < half, re, moved).T
        table_t[LANES:width, at:at + LANES] = moved.T[0:width - LANES, :]


def bucket_kernel(shift, group, used, h_ids, r_ids, tail_ids, table_hbm, rel, r_vec, tail_vec,
                  gh_out, gt_out, gn_out, grel_ref, loss_ref,
                  table, gh_ref, gt_ref, gn_ref, h_rows, r_rows, t_rows, n_rows, n_bf, gn_acc, table_sem, gh_sems, gt_sems, *scratch):
    edges = h_rows.shape[0] // 2
    negs = n_bf.shape[0]
    sent = 2 * EDGE_BLOCK * used // LANES
    load = pltpu.make_async_copy(table_hbm, table, table_sem.at[0])
    load.start()
    rel_pad = grel_ref.shape[0] // 2
    steps = edges // EDGE_BLOCK

    def block(step):
        return pl.ds(pl.multiple_of(step * EDGE_BLOCK, EDGE_BLOCK), EDGE_BLOCK)

    def halves(base, count):
        return pl.ds(pl.multiple_of(2 * base, 2), count, stride=2), pl.ds(2 * base + 1, count, stride=2)

    def wire(step):
        return pl.ds(pl.multiple_of(step * sent, sent), sent)

    def out_copy(src, dst, sems, step):
        rows = pl.ds(pl.multiple_of(2 * step * EDGE_BLOCK, 2 * EDGE_BLOCK), 2 * EDGE_BLOCK)
        return pltpu.make_async_copy(src.at[rows, :], dst.at[rows, :], sems.at[step])

    gn_copy = pltpu.make_async_copy(gn_ref, gn_out, table_sem.at[1])

    if shift:
        q_own, q_got, gq_send, gq_got, loss_send, q_sems, gq_sems, loss_sems = scratch
        me = lax.axis_index('ent')
        ahead = lax.rem(me + shift, group)
        behind = lax.rem(me + group - shift, group)

        def q_copy(step):
            return pltpu.make_async_remote_copy(
                src_ref=q_own.at[wire(step), :], dst_ref=q_got.at[wire(step), :],
                send_sem=q_sems.at[0, step], recv_sem=q_sems.at[1, step],
                device_id={'ent': ahead}, device_id_type=MESH)

        def gq_copy(step):
            return pltpu.make_async_remote_copy(
                src_ref=gq_send.at[wire(step), :], dst_ref=gq_got.at[wire(step), :],
                send_sem=gq_sems.at[0, step], recv_sem=gq_sems.at[1, step],
                device_id={'ent': behind}, device_id_type=MESH)

        barrier = pltpu.get_barrier_semaphore()
        pl.semaphore_signal(barrier, inc=1, device_id={'ent': ahead}, device_id_type=MESH)
        pl.semaphore_signal(barrier, inc=1, device_id={'ent': behind}, device_id_type=MESH)
        pl.semaphore_wait(barrier, 2)
    else:
        q_own, gq_got = scratch
    load.wait()

    def ask(step, _):
        def gather(part, _):
            base = step * EDGE_BLOCK + part * GATHER_UNROLL
            for off in range(GATHER_UNROLL):
                at = base + off
                h_rows[pair(at), :] = table[h_ids[shift, at]]
            return 0

        def gather_rel(part, _):
            base = step * EDGE_BLOCK + part * GATHER_UNROLL
            for off in range(GATHER_UNROLL):
                at = base + off
                r_rows[pair(at), :] = rel[r_ids[shift, at]]
            return 0

        lax.fori_loop(0, EDGE_BLOCK // GATHER_UNROLL, gather, 0)
        lax.fori_loop(0, EDGE_BLOCK // GATHER_UNROLL, gather_rel, 0)
        even, odd = halves(step * EDGE_BLOCK, EDGE_BLOCK)
        re_h, im_h = h_rows[even, :], h_rows[odd, :]
        re_r, im_r = r_rows[even, :], r_rows[odd, :]
        re_q, im_q = re_h * re_r - im_h * im_r, re_h * im_r + im_h * re_r
        if shift:
            q_own[wire(step), :] = pack_rows(used, jnp.concatenate([re_q, im_q], axis=0)).astype(BF16)
            q_copy(step).start()
        else:
            q_own[block(step), :] = jnp.concatenate([re_q, im_q], axis=1).astype(BF16)
        return 0

    lax.fori_loop(0, steps, ask, 0)

    def gather_negs(part, _):
        for off in range(GATHER_UNROLL):
            at = part * GATHER_UNROLL + off
            n_rows[pair(at), :] = table[tail_ids[0, 2 * edges + at]]
        return 0

    lax.fori_loop(0, negs // GATHER_UNROLL, gather_negs, 0)
    n_even, n_odd = halves(0, negs)
    n_bf[:, 0:LANES] = n_rows[n_even, :].astype(BF16)
    n_bf[:, LANES:2 * LANES] = n_rows[n_odd, :].astype(BF16)

    def gather_tails(part, _):
        for off in range(GATHER_UNROLL):
            at = part * GATHER_UNROLL + off
            t_rows[pair(at), :] = table[tail_ids[0, at]]
        return 0

    lax.fori_loop(0, edges // GATHER_UNROLL, gather_tails, 0)

    gn_acc[...] = jnp.zeros_like(gn_acc)
    eye = lax.broadcasted_iota(jnp.int32, (LANES, LANES), 0) == lax.broadcasted_iota(jnp.int32, (LANES, LANES), 1)
    per_block = EDGE_BLOCK // LANES

    def answer(step, loss_acc):
        if shift:
            q_copy(step).wait_recv()
        even, odd = halves(step * EDGE_BLOCK, EDGE_BLOCK)
        if shift:
            wide = unpack_rows(used, 2 * EDGE_BLOCK, q_got[wire(step), :].astype(F32))
            q = jnp.concatenate([wide[:EDGE_BLOCK], wide[EDGE_BLOCK:]], axis=1).astype(BF16)
        else:
            q = q_own[block(step), :]
        t = jnp.concatenate([t_rows[even, :].astype(BF16), t_rows[odd, :].astype(BF16)], axis=1).astype(F32)
        q_wide = q.astype(F32)
        n = n_bf[...]
        masks = [tail_vec[0:1, pl.ds(pl.multiple_of(edges + step * EDGE_BLOCK + k * LANES, LANES), LANES)].astype(F32) for k in range(per_block)]
        w = jnp.concatenate([jnp.sum(jnp.where(eye, mask, 0.0), axis=1, keepdims=True) for mask in masks], axis=0)
        pos = jnp.sum(q_wide * t, axis=1, keepdims=True)
        score = lax.dot_general(q, n, (((1,), (1,)), ((), ())), preferred_element_type=F32)
        top = jnp.maximum(jnp.max(score, axis=1, keepdims=True), pos)
        pos_exp = jnp.exp(pos - top)
        neg_exp = jnp.exp(score - top)
        total = pos_exp + jnp.sum(neg_exp, axis=1, keepdims=True)
        loss_acc = loss_acc + jnp.sum(w * (top + jnp.log(total) - pos), axis=0, keepdims=True)
        d_pos = w * (pos_exp / total - 1.0)
        d_neg = ((w / total) * neg_exp).astype(BF16)
        g_q = d_pos * t + jnp.dot(d_neg, n, preferred_element_type=F32)
        g_tail = d_pos * q_wide
        gt_ref[even, :] = g_tail[:, 0:LANES]
        gt_ref[odd, :] = g_tail[:, LANES:2 * LANES]
        gn_acc[...] += lax.dot_general(q, d_neg, (((0,), (0,)), ((), ())), preferred_element_type=F32)
        if shift:
            gq_send[wire(step), :] = pack_rows(used, jnp.concatenate([g_q[:, 0:LANES], g_q[:, LANES:2 * LANES]], axis=0)).astype(BF16)
            gq_copy(step).start()
        else:
            gq_got[block(step), :] = g_q
        out_copy(gt_ref, gt_out, gt_sems, step).start()
        return loss_acc

    loss = lax.fori_loop(0, steps, answer, jnp.zeros((1, 1), F32))
    if shift:
        loss_send[...] = jnp.broadcast_to(loss, loss_send.shape)
        loss_copy = pltpu.make_async_remote_copy(
            src_ref=loss_send, dst_ref=loss_ref, send_sem=loss_sems.at[0], recv_sem=loss_sems.at[1],
            device_id={'ent': behind}, device_id_type=MESH)
        loss_copy.start()
    else:
        loss_ref[...] = jnp.broadcast_to(loss, loss_ref.shape)
    for half in range(2):
        gn_ref[pl.ds(half, negs, stride=2), :] = gn_acc[half * LANES:(half + 1) * LANES, :].T
    gn_copy.start()

    def finish(step, carry):
        rel_re, rel_im = carry
        if shift:
            gq_copy(step).wait_recv()
            wide = unpack_rows(used, 2 * EDGE_BLOCK, gq_got[wire(step), :].astype(F32))
            re_g, im_g = wide[:EDGE_BLOCK], wide[EDGE_BLOCK:]
        else:
            re_g, im_g = gq_got[block(step), 0:LANES], gq_got[block(step), LANES:2 * LANES]
        even, odd = halves(step * EDGE_BLOCK, EDGE_BLOCK)
        re_r, im_r = r_rows[even, :], r_rows[odd, :]
        gh_ref[even, :] = re_g * re_r + im_g * im_r
        gh_ref[odd, :] = im_g * re_r - re_g * im_r
        out_copy(gh_ref, gh_out, gh_sems, step).start()
        re_h, im_h = h_rows[even, :], h_rows[odd, :]
        ids = r_vec[shift:shift + 1, pl.ds(pl.multiple_of(step * EDGE_BLOCK, EDGE_BLOCK), EDGE_BLOCK)]
        hot = (lax.broadcasted_iota(jnp.int32, (rel_pad, EDGE_BLOCK), 0) == ids).astype(F32)
        rel_re = rel_re + jnp.dot(hot, re_g * re_h + im_g * im_h, precision=lax.Precision.HIGHEST, preferred_element_type=F32)
        rel_im = rel_im + jnp.dot(hot, im_g * re_h - re_g * im_h, precision=lax.Precision.HIGHEST, preferred_element_type=F32)
        return rel_re, rel_im

    zero = jnp.zeros((rel_pad, LANES), F32)
    rel_re, rel_im = lax.fori_loop(0, steps, finish, (zero, zero))
    grel_ref[pl.ds(0, rel_pad, stride=2), :] = rel_re
    grel_ref[pl.ds(1, rel_pad, stride=2), :] = rel_im
    if shift:
        loss_copy.wait()
    gn_copy.wait()

    def drain(step, _):
        if shift:
            q_copy(step).wait_send()
            gq_copy(step).wait_send()
        out_copy(gt_ref, gt_out, gt_sems, step).wait()
        out_copy(gh_ref, gh_out, gh_sems, step).wait()
        return 0

    lax.fori_loop(0, steps, drain, 0)


def scatter_kernel(shift, h_ids, tail_ids, gh_in, gt_in, gn_in, acc_out, acc, acc_b, acc_c, acc_d, gh, gt_ref, gn_ref, in_sems, out_sems):
    edges = gh.shape[0] // 2
    negs = gn_ref.shape[0] // 2
    table_rows = acc.shape[0]
    zero_rows = 512
    pieces = 8
    piece = table_rows // pieces

    copies = [pltpu.make_async_copy(src, dst, in_sems.at[at]) for at, (src, dst) in enumerate(((gh_in, gh), (gt_in, gt_ref), (gn_in, gn_ref)))]
    for copy in copies:
        copy.start()

    def clear(step, _):
        rows = pl.ds(pl.multiple_of(step * zero_rows, zero_rows), zero_rows)
        for ref in (acc, acc_b, acc_c, acc_d):
            ref[rows, :] = jnp.zeros((zero_rows, LANES), F32)
        return 0

    lax.fori_loop(0, table_rows // zero_rows, clear, 0)
    for copy in copies:
        copy.wait()

    def add_edges(step, _):
        base = step * SCATTER_UNROLL
        for off in range(0, SCATTER_UNROLL, 2):
            at = base + off
            places = (pair(h_ids[shift, at]), pair(h_ids[shift, at + 1]), pair(tail_ids[0, at]), pair(tail_ids[0, at + 1]))
            refs = (acc, acc_b, acc_c, acc_d)
            terms = (gh[pair(at), :], gh[pair(at + 1), :], gt_ref[pair(at), :], gt_ref[pair(at + 1), :])
            sums = [ref[place, :] + term for ref, place, term in zip(refs, places, terms)]
            for ref, place, total in zip(refs, places, sums):
                ref[place, :] = total
        return 0

    lax.fori_loop(0, edges // SCATTER_UNROLL, add_edges, 0)

    def add_negs(step, _):
        base = step * SCATTER_UNROLL
        for off in range(0, SCATTER_UNROLL, 4):
            at = base + off
            places = [pair(tail_ids[0, 2 * edges + at + k]) for k in range(4)]
            refs = (acc, acc_b, acc_c, acc_d)
            sums = [ref[place, :] + gn_ref[pair(at + k), :] for k, (ref, place) in enumerate(zip(refs, places))]
            for ref, place, total in zip(refs, places, sums):
                ref[place, :] = total
        return 0

    lax.fori_loop(0, negs // SCATTER_UNROLL, add_negs, 0)

    def out_copy(at):
        rows = pl.ds(pl.multiple_of(at * piece, piece), piece)
        return pltpu.make_async_copy(acc.at[rows, :], acc_out.at[rows, :], out_sems.at[at])

    def combine(at, _):
        rows = pl.ds(pl.multiple_of(at * piece, piece), piece)
        acc[rows, :] = (acc[rows, :] + acc_b[rows, :]) + (acc_c[rows, :] + acc_d[rows, :])
        out_copy(at).start()
        return 0

    lax.fori_loop(0, pieces, combine, 0)
    for at in range(pieces):
        out_copy(at).wait()


def pieces_of(half):
    found, at = [], 0
    for bit in range(7, -1, -1):
        if half >> bit & 1:
            found.append((1 << bit, at))
            at += 1 << bit
    return found


def pack_rows(half, x):
    n = x.shape[0]
    lane = lax.broadcasted_iota(jnp.int32, (1, LANES), 1)
    out = []
    for size, at in pieces_of(half):
        groups = LANES // size
        rows = n // groups
        acc = None
        for k in range(groups):
            part = pltpu.roll(x[k * rows:(k + 1) * rows], (k * size - at) % LANES, 1)
            acc = part if acc is None else jnp.where(lane < k * size, acc, part)
        out.append(acc)
    return jnp.concatenate(out, axis=0)


def unpack_rows(half, n, x):
    lane = lax.broadcasted_iota(jnp.int32, (1, LANES), 1)
    out, start = None, 0
    for size, at in pieces_of(half):
        groups = LANES // size
        rows = n // groups
        block = x[start:start + rows]
        start += rows
        parts = jnp.concatenate([pltpu.roll(block, (at - k * size) % LANES, 1) for k in range(groups)], axis=0)
        out = parts if out is None else jnp.where(lane < at, out, parts)
    return jnp.where(lane < half, out, 0.0)


def update_kernel(width, learn_rate, groups, reps, shift, bucket_edges, acc_hbm, table_hbm, state_in, grel_in, rel_in, rel_state_in, loss_in, losses_in,
                  table_out, state_out, rel_out, rel_state_out, losses_out, state_all,
                  acc, table, first_send, first_got, plain_send, plain_got, merged_send, merged_got, work,
                  step_own, step_got, step_far, rel_x, rel_y, rel_send, rel_send_y, state_own, acc_sems, table_sems, out_sems,
                  first_sems, plain_sems, merged_sems, own_sems, far_sems, rel_x_sems, rel_y_sems, state_sems):
    me = lax.axis_index('data')
    ent = lax.axis_index('ent')
    used = width // 2
    peers = (lax.rem(me + 1, reps), lax.rem(me + reps - 1, reps))
    peer_slots = (1, reps - 1)
    half = acc.shape[2]
    chunk = half // SYNC_CHUNKS
    sent = chunk * used // LANES

    def part_rows(slot, which):
        return pl.ds(pl.multiple_of((lax.rem(me + slot, reps) * 2 + which) * half, half), half)

    def load(src, dst, sems, slot, which):
        return pltpu.make_async_copy(src.at[part_rows(slot, which), :], dst.at[slot, which], sems.at[slot, which])

    def save(slot, which):
        return pltpu.make_async_copy(table.at[slot, which], table_out.at[part_rows(slot, which), :], out_sems.at[slot, which])

    for slot, which in ((2, 0), (2, 1), (1, 1), (3, 0), (1, 0), (3, 1), (0, 0), (0, 1)):
        load(acc_hbm, acc, acc_sems, slot, which).start()
    for slot in range(reps):
        for which in range(2):
            load(table_hbm, table, table_sems, slot, which).start()

    barrier = pltpu.get_barrier_semaphore()
    for off in range(1, reps):
        pl.semaphore_signal(barrier, inc=1, device_id={'data': lax.rem(me + off, reps)}, device_id_type=MESH)
    for off in range(1, groups):
        pl.semaphore_signal(barrier, inc=1, device_id={'ent': lax.rem(ent + off, groups)}, device_id_type=MESH)
    pl.semaphore_wait(barrier, reps + groups - 2)

    def remote(src, dst, sems, place, to):
        return pltpu.make_async_remote_copy(
            src_ref=src, dst_ref=dst, send_sem=sems.at[(0,) + place], recv_sem=sems.at[(1,) + place],
            device_id=to, device_id_type=MESH)

    rel_x[0] = grel_in[...]
    rel_send[...] = grel_in[...]
    x_copies = [remote(rel_send, rel_x.at[off], rel_x_sems, (off - 1,), {'ent': lax.rem(ent + off, groups)}) for off in range(1, groups)]
    for copy in x_copies:
        copy.start()

    def at_chunk(k):
        return pl.ds(pl.multiple_of(k * chunk, chunk), chunk)

    def at_sent(k):
        return pl.ds(pl.multiple_of(k * sent, sent), sent)

    def first(side, k):
        return remote(first_send.at[side, at_sent(k), :], first_got.at[side, at_sent(k), :], first_sems, (side, k), {'data': peers[side]})

    def plain(side, k):
        return remote(plain_send.at[side, at_sent(k), :], plain_got.at[side, at_sent(k), :], plain_sems, (side, k), {'data': peers[side]})

    def merged(side, k):
        return remote(merged_send.at[side, at_sent(k), :], merged_got.at[side, at_sent(k), :], merged_sems, (side, k), {'data': peers[side]})

    def own(side, which, k):
        return remote(step_own.at[which, at_sent(k), :], step_got.at[side, which, at_sent(k), :], own_sems, (side, which, k), {'data': peers[side]})

    def spread(side, k):
        return remote(step_got.at[side, side, at_sent(k), :], step_far.at[side, at_sent(k), :], far_sems, (side, k), {'data': peers[side]})

    def send_first(k, _):
        for side in range(2):
            first_send[side, at_sent(k), :] = pack_rows(used, acc[2, side, at_chunk(k), :]).astype(BF16)
            first(side, k).start()
        return 0

    def send_plain(k, _):
        for side in range(2):
            plain_send[side, at_sent(k), :] = pack_rows(used, acc[peer_slots[side], 1 - side, at_chunk(k), :]).astype(BF16)
            plain(side, k).start()
        return 0

    def send_merged(k, _):
        for side in range(2):
            first(side, k).wait_recv()
            merged_send[side, at_sent(k), :] = (first_got[side, at_sent(k), :].astype(F32) + pack_rows(used, acc[peer_slots[side], side, at_chunk(k), :])).astype(BF16)
            merged(side, k).start()
        return 0

    for needed, body in ((((2, 0), (2, 1)), send_first), (((1, 1), (3, 0)), send_plain), (((1, 0), (3, 1)), send_merged)):
        for slot, which in needed:
            load(acc_hbm, acc, acc_sems, slot, which).wait()
        lax.fori_loop(0, SYNC_CHUNKS, body, 0)

    for copy in x_copies:
        copy.wait()
    total = rel_x[lax.rem(ent, groups)]
    for src in range(1, groups):
        total = total + rel_x[lax.rem(ent + groups - src, groups)]
    span = total.shape[0]
    rel_send_y[0:span, :] = total
    rel_send_y[span:, :] = loss_in[...]
    rel_y[0] = rel_send_y[...]
    y_copies = [remote(rel_send_y, rel_y.at[off], rel_y_sems, (off - 1,), {'data': lax.rem(me + off, reps)}) for off in range(1, reps)]
    for copy in y_copies:
        copy.start()

    for which in range(2):
        load(acc_hbm, acc, acc_sems, 0, which).wait()
    for slot in range(reps):
        for which in range(2):
            load(table_hbm, table, table_sems, slot, which).wait()
    n = chunk // 2
    even, odd = pl.ds(0, n, stride=2), pl.ds(1, n, stride=2)

    def step_rows(k, _):
        for which in range(2):
            merged(which, k).wait_recv()
            plain(1 - which, k).wait_recv()
            others = merged_got[which, at_sent(k), :].astype(F32) + plain_got[1 - which, at_sent(k), :].astype(F32)
            work[...] = acc[0, which, at_chunk(k), :] + unpack_rows(used, chunk, others)
            re_g, im_g = work[even, :], work[odd, :]
            places = pl.ds(pl.multiple_of(which * (half // 2) + k * n, n), n)
            state = state_in[places, :] + jnp.sum(re_g * re_g + im_g * im_g, axis=1, keepdims=True) / width
            state_out[places, :] = state
            scale = learn_rate / jnp.sqrt(state + EPSILON)
            work[even, :] = re_g * scale
            work[odd, :] = im_g * scale
            moves = work[...]
            step_own[which, at_sent(k), :] = pack_rows(used, moves).astype(BF16)
            for side in range(2):
                own(side, which, k).start()
            table[0, which, at_chunk(k), :] -= moves.astype(BF16).astype(F32)
        return 0

    lax.fori_loop(0, SYNC_CHUNKS, step_rows, 0)
    for which in range(2):
        save(0, which).start()

    def take_near(k, _):
        for which in range(2):
            for side in (which, 1 - which):
                own(side, which, k).wait_recv()
                if side == which:
                    spread(side, k).start()
                table[peer_slots[1 - side], which, at_chunk(k), :] -= unpack_rows(used, chunk, step_got[side, which, at_sent(k), :].astype(F32))
        return 0

    lax.fori_loop(0, SYNC_CHUNKS, take_near, 0)
    for slot in peer_slots:
        for which in range(2):
            save(slot, which).start()

    for copy in y_copies:
        copy.wait()
    total = rel_y[lax.rem(me, reps)]
    for src in range(1, reps):
        total = total + rel_y[lax.rem(me + reps - src, reps)]
    losses_out[...] = jnp.where(lax.broadcasted_iota(jnp.int32, losses_in.shape, 0) == shift, total[span:, :] / bucket_edges, losses_in[...])
    rel_send[...] = total[0:span, :]
    rel_rows = rel_send.shape[0] // 2
    re_g, im_g = rel_send[pl.ds(0, rel_rows, stride=2), :], rel_send[pl.ds(1, rel_rows, stride=2), :]
    state = rel_state_in[...] + jnp.sum(re_g * re_g + im_g * im_g, axis=1, keepdims=True) / width
    rel_state_out[...] = state
    scale = learn_rate / jnp.sqrt(state + EPSILON)
    rel_out[pl.ds(0, rel_rows, stride=2), :] = rel_in[pl.ds(0, rel_rows, stride=2), :] - re_g * scale
    rel_out[pl.ds(1, rel_rows, stride=2), :] = rel_in[pl.ds(1, rel_rows, stride=2), :] - im_g * scale

    state_copies = []
    if shift == groups - 1:
        eye = lax.broadcasted_iota(jnp.int32, (LANES, LANES), 0) == lax.broadcasted_iota(jnp.int32, (LANES, LANES), 1)
        blocks = state_own.shape[0]
        for at in range(blocks):
            state_own[at:at + 1, :] = jnp.sum(jnp.where(eye, state_out[at * LANES:(at + 1) * LANES, :], 0.0), axis=0, keepdims=True)
        place = pl.ds(pl.multiple_of(me * blocks, blocks), blocks)
        state_all[place, :] = state_own[...]
        state_copies = [remote(state_own, state_all.at[place, :], state_sems, (off - 1,), {'data': lax.rem(me + off, reps)}) for off in range(1, reps)]
        for copy in state_copies:
            copy.start()
    else:
        state_all[...] = jnp.zeros_like(state_all)

    def take_far(k, _):
        for side in range(2):
            spread(side, k).wait_recv()
            table[2, side, at_chunk(k), :] -= unpack_rows(used, chunk, step_far[side, at_sent(k), :].astype(F32))
        return 0

    lax.fori_loop(0, SYNC_CHUNKS, take_far, 0)
    for which in range(2):
        save(2, which).start()

    def drain(k, _):
        for side in range(2):
            for copy in (first(side, k), plain(side, k), merged(side, k), own(side, 0, k), own(side, 1, k), spread(side, k)):
                copy.wait_send()
        return 0

    lax.fori_loop(0, SYNC_CHUNKS, drain, 0)
    for slot in range(reps):
        for which in range(2):
            save(slot, which).wait()
    for copy in state_copies:
        copy.wait()


def solution(mesh):
    groups = mesh.shape['ent']
    reps = mesh.shape['data']
    row_spec = P(('sweep', 'ent'), None)
    edge_spec = P(('sweep', 'ent'), None, 'data')
    vmem = pl.BlockSpec(memory_space=VM)

    def device_fn(ent_table, ent_state, rel_table, head_idx, tail_idx, rel_idx, edge_mask, neg_idx):
        part_rows, width = ent_table.shape
        rel_count = rel_table.shape[0]
        edges = head_idx.shape[2]
        negs = neg_idx.shape[2]
        bucket_edges = edges * reps
        learn_rate = LR_SCALE * width ** -0.25
        rel_pad = -(-rel_count // 8) * 8
        quarter = part_rows // reps
        me = lax.axis_index('data')

        packed = jnp.concatenate([tail_idx[0], edge_mask[0], neg_idx[0]], axis=1)
        moved = [packed[0:1]]
        for shift in range(1, groups):
            moved.append(lax.ppermute(packed[shift:shift + 1], 'ent', [(src, (src + shift) % groups) for src in range(groups)]))

        h_all = head_idx[0]
        r_all = rel_idx[0]
        row_grid = 8
        params = pltpu.CompilerParams(vmem_limit_bytes=VMEM_LIMIT)
        table = pl.pallas_call(
            functools.partial(load_kernel, width // 2), grid=(row_grid,),
            out_shape=jax.ShapeDtypeStruct((2 * part_rows, LANES), F32),
            in_specs=[pl.BlockSpec((width, part_rows // row_grid), lambda i: (0, i))],
            out_specs=pl.BlockSpec((2 * part_rows // row_grid, LANES), lambda i: (i, 0)),
            scratch_shapes=[VM((2 * LANES, part_rows // row_grid), F32)], name='load_table')(ent_table.T)
        rel = interleave(jnp.pad(rel_table, ((0, rel_pad - rel_count), (0, 0))))
        rel_state = jnp.zeros((rel_pad, LANES), F32)
        state = jnp.broadcast_to(lax.dynamic_slice_in_dim(ent_state, me * quarter, quarter)[:, None], (quarter, LANES))
        losses = jnp.zeros((-(-groups // 8) * 8, LANES), F32)

        smem = pl.BlockSpec(memory_space=pltpu.SMEM)
        hbm = pl.BlockSpec(memory_space=pl.ANY)
        sems = pltpu.SemaphoreType.DMA
        steps = edges // EDGE_BLOCK
        for shift in range(groups):
            tail = moved[shift]
            scratch = [VM((part_rows, 2, LANES), F32)] + [VM((2 * edges, LANES), F32)] * 2 + [VM((2 * negs, LANES), F32)]
            scratch += [VM((2 * edges, LANES), F32)] * 3 + [VM((2 * negs, LANES), F32), VM((negs, 2 * LANES), BF16), VM((2 * LANES, negs), F32)]
            scratch += [sems((2,)), sems((steps,)), sems((steps,))]
            if shift:
                scratch += [VM((2 * edges * (width // 2) // LANES, LANES), BF16)] * 4 + [VM(losses.shape, F32), sems((2, steps)), sems((2, steps)), sems((2,))]
            else:
                scratch += [VM((edges, 2 * LANES), BF16), VM((edges, 2 * LANES), F32)]
            g_h, g_t, g_n, g_rel, loss = pl.pallas_call(
                functools.partial(bucket_kernel, shift, groups, width // 2),
                out_shape=[jax.ShapeDtypeStruct((2 * edges, LANES), F32)] * 2
                + [jax.ShapeDtypeStruct((2 * negs, LANES), F32), jax.ShapeDtypeStruct((2 * rel_pad, LANES), F32), jax.ShapeDtypeStruct(losses.shape, F32)],
                in_specs=[smem] * 3 + [hbm] + [vmem] * 3, out_specs=[hbm] * 3 + [vmem] * 2, scratch_shapes=scratch,
                compiler_params=pltpu.CompilerParams(vmem_limit_bytes=VMEM_LIMIT, collective_id=0, has_side_effects=True) if shift else params,
                name='bucket',
            )(h_all, r_all, tail, table.reshape(part_rows, 2, LANES), rel.reshape(rel_pad, 2, LANES), r_all, tail)

            acc = pl.pallas_call(
                functools.partial(scatter_kernel, shift),
                out_shape=jax.ShapeDtypeStruct((2 * part_rows, LANES), F32),
                in_specs=[smem] * 2 + [hbm] * 3, out_specs=hbm,
                scratch_shapes=[VM((2 * part_rows, LANES), F32)] * 4 + [VM((2 * edges, LANES), F32)] * 2 + [VM((2 * negs, LANES), F32), sems((3,)), sems((8,))],
                compiler_params=params, name='scatter_rows',
            )(h_all, tail, g_h, g_t, g_n)

            half = (2 * part_rows) // reps // 2
            half_sent = half * (width // 2) // LANES
            block = VM((2, half_sent, LANES), BF16)
            state_blocks = quarter // LANES
            table, state, rel, rel_state, losses, state_all = pl.pallas_call(
                functools.partial(update_kernel, width, learn_rate, groups, reps, shift, bucket_edges),
                out_shape=[jax.ShapeDtypeStruct(table.shape, F32), jax.ShapeDtypeStruct(state.shape, F32),
                           jax.ShapeDtypeStruct(rel.shape, F32), jax.ShapeDtypeStruct(rel_state.shape, F32),
                           jax.ShapeDtypeStruct(losses.shape, F32), jax.ShapeDtypeStruct((reps * state_blocks, LANES), F32)],
                in_specs=[hbm] * 2 + [vmem] * 6, out_specs=[hbm] + [vmem] * 5,
                scratch_shapes=[VM((reps, 2, half, LANES), F32)] * 2 + [block] * 6 + [VM((half // SYNC_CHUNKS, LANES), F32), block, VM((2, 2, half_sent, LANES), BF16), block,
                                              VM((groups, 2 * rel_pad, LANES), F32), VM((reps, 2 * rel_pad + losses.shape[0], LANES), F32), VM((2 * rel_pad, LANES), F32),
                                              VM((2 * rel_pad + losses.shape[0], LANES), F32), VM((state_blocks, LANES), F32), sems((reps, 2)), sems((reps, 2)), sems((reps, 2)),
                                              sems((2, 2, SYNC_CHUNKS)), sems((2, 2, SYNC_CHUNKS)), sems((2, 2, SYNC_CHUNKS)),
                                              sems((2, 2, 2, SYNC_CHUNKS)), sems((2, 2, SYNC_CHUNKS)), sems((2, groups - 1)), sems((2, reps - 1)), sems((2, reps - 1))],
                compiler_params=pltpu.CompilerParams(vmem_limit_bytes=VMEM_LIMIT, collective_id=1, has_side_effects=True), name='update',
            )(acc, table, state, g_rel, rel, rel_state, loss, losses)

        ent_out = pl.pallas_call(
            functools.partial(store_kernel, width // 2), grid=(row_grid,),
            out_shape=jax.ShapeDtypeStruct((width, part_rows), F32),
            in_specs=[pl.BlockSpec((2 * part_rows // row_grid, LANES), lambda i: (i, 0))],
            out_specs=pl.BlockSpec((width, part_rows // row_grid), lambda i: (0, i)), name='store_table')(table).T
        rel_out = deinterleave(rel, width)[:rel_count]
        return ent_out, state_all.reshape(part_rows), rel_out, losses[:groups, 0].reshape(1, groups)

    return jax.shard_map(device_fn, mesh=mesh, in_specs=(row_spec, P(('sweep', 'ent')), P('sweep', None), edge_spec, edge_spec, edge_spec, edge_spec, P(('sweep', 'ent'), None, None)), out_specs=(row_spec, P(('sweep', 'ent')), P('sweep', None), row_spec), check_vma=False)
```

```python
import functools

import jax
import jax.numpy as jnp
from jax import lax
from jax.experimental import pallas as pl
from jax.experimental.pallas import tpu as pltpu
from jax.sharding import PartitionSpec as P

LR_SCALE = 0.2
EPSILON = 1e-8
LANES = 128
EDGE_BLOCK = 256
GATHER_UNROLL = 32
SCATTER_UNROLL = 16
SYNC_CHUNKS = 4
VMEM_LIMIT = 60 * 1024 * 1024
MESH = pl.DeviceIdType.MESH
VM = pltpu.VMEM
F32 = jnp.float32
BF16 = jnp.bfloat16


def interleave(table):
    rows, width = table.shape
    half = width // 2
    return jnp.pad(table.reshape(rows, 2, half), ((0, 0), (0, 0), (0, LANES - half))).reshape(rows * 2, LANES)


def deinterleave(table, width):
    rows = table.shape[0] // 2
    return table.reshape(rows, 2, LANES)[:, :, :width // 2].reshape(rows, width)


def pair(row):
    return pl.ds(pl.multiple_of(row * 2, 2), 2)


def load_kernel(half, table_t, table, staged):
    width, cols = table_t.shape
    staged[0:width, :] = table_t[...]
    staged[width:2 * LANES, :] = jnp.zeros((2 * LANES - width, cols), F32)
    lane = lax.broadcasted_iota(jnp.int32, (LANES, LANES), 1)
    for at in range(0, cols, LANES):
        low = staged[0:LANES, at:at + LANES].T
        high = staged[LANES:2 * LANES, at:at + LANES].T
        table[pl.ds(2 * at, LANES, stride=2), :] = jnp.where(lane < half, low, 0.0)
        moved = jnp.where(lane < LANES - half, pltpu.roll(low, LANES - half, 1), pltpu.roll(high, LANES - half, 1))
        table[pl.ds(2 * at + 1, LANES, stride=2), :] = jnp.where(lane < half, moved, 0.0)


def store_kernel(half, table, table_t):
    width, cols = table_t.shape
    lane = lax.broadcasted_iota(jnp.int32, (LANES, LANES), 1)
    for at in range(0, cols, LANES):
        re = table[pl.ds(2 * at, LANES, stride=2), :]
        moved = pltpu.roll(table[pl.ds(2 * at + 1, LANES, stride=2), :], half, 1)
        table_t[0:LANES, at:at + LANES] = jnp.where(lane < half, re, moved).T
        table_t[LANES:width, at:at + LANES] = moved.T[0:width - LANES, :]


def bucket_kernel(shift, group, used, head_ids, tail_ids, table_hbm, rel, head_vec, tail_vec,
                  gh_out, gt_out, gn_out, grel_ref, loss_ref,
                  table, gh_ref, gt_ref, gn_ref, h_rows, r_rows, t_rows, n_rows, n_bf, gn_acc, table_sem, gh_sems, gt_sems, *scratch):
    edges = h_rows.shape[0] // 2
    negs = n_bf.shape[0]
    sent = 2 * EDGE_BLOCK * used // LANES
    load = pltpu.make_async_copy(table_hbm, table, table_sem.at[0])
    load.start()
    rel_pad = grel_ref.shape[0] // 2
    steps = edges // EDGE_BLOCK

    def block(step):
        return pl.ds(pl.multiple_of(step * EDGE_BLOCK, EDGE_BLOCK), EDGE_BLOCK)

    def halves(base, count):
        return pl.ds(pl.multiple_of(2 * base, 2), count, stride=2), pl.ds(2 * base + 1, count, stride=2)

    def wire(step):
        return pl.ds(pl.multiple_of(step * sent, sent), sent)

    def out_copy(src, dst, sems, step):
        rows = pl.ds(pl.multiple_of(2 * step * EDGE_BLOCK, 2 * EDGE_BLOCK), 2 * EDGE_BLOCK)
        return pltpu.make_async_copy(src.at[rows, :], dst.at[rows, :], sems.at[step])

    gn_copy = pltpu.make_async_copy(gn_ref, gn_out, table_sem.at[1])

    if shift:
        q_own, q_got, gq_send, gq_got, loss_send, q_sems, gq_sems, loss_sems = scratch
        me = lax.axis_index('ent')
        ahead = lax.rem(me + shift, group)
        behind = lax.rem(me + group - shift, group)

        def q_copy(step):
            return pltpu.make_async_remote_copy(
                src_ref=q_own.at[wire(step), :], dst_ref=q_got.at[wire(step), :],
                send_sem=q_sems.at[0, step], recv_sem=q_sems.at[1, step],
                device_id={'ent': ahead}, device_id_type=MESH)

        def gq_copy(step):
            return pltpu.make_async_remote_copy(
                src_ref=gq_send.at[wire(step), :], dst_ref=gq_got.at[wire(step), :],
                send_sem=gq_sems.at[0, step], recv_sem=gq_sems.at[1, step],
                device_id={'ent': behind}, device_id_type=MESH)

        barrier = pltpu.get_barrier_semaphore()
        pl.semaphore_signal(barrier, inc=1, device_id={'ent': ahead}, device_id_type=MESH)
        pl.semaphore_signal(barrier, inc=1, device_id={'ent': behind}, device_id_type=MESH)
        pl.semaphore_wait(barrier, 2)
    else:
        q_own, gq_got = scratch
    load.wait()

    def ask(step, _):
        def gather(part, _):
            base = step * EDGE_BLOCK + part * GATHER_UNROLL
            for off in range(GATHER_UNROLL):
                at = base + off
                h_rows[pair(at), :] = table[head_ids[0, at]]
            return 0

        def gather_rel(part, _):
            base = step * EDGE_BLOCK + part * GATHER_UNROLL
            for off in range(GATHER_UNROLL):
                at = base + off
                r_rows[pair(at), :] = rel[head_ids[0, edges + at]]
            return 0

        lax.fori_loop(0, EDGE_BLOCK // GATHER_UNROLL, gather, 0)
        lax.fori_loop(0, EDGE_BLOCK // GATHER_UNROLL, gather_rel, 0)
        even, odd = halves(step * EDGE_BLOCK, EDGE_BLOCK)
        re_h, im_h = h_rows[even, :], h_rows[odd, :]
        re_r, im_r = r_rows[even, :], r_rows[odd, :]
        re_q, im_q = re_h * re_r - im_h * im_r, re_h * im_r + im_h * re_r
        if shift:
            q_own[wire(step), :] = pack_rows(used, jnp.concatenate([re_q, im_q], axis=0)).astype(BF16)
            q_copy(step).start()
        else:
            q_own[block(step), :] = jnp.concatenate([re_q, im_q], axis=1).astype(BF16)
        return 0

    lax.fori_loop(0, steps, ask, 0)

    def gather_negs(part, _):
        for off in range(GATHER_UNROLL):
            at = part * GATHER_UNROLL + off
            n_rows[pair(at), :] = table[tail_ids[0, 2 * edges + at]]
        return 0

    lax.fori_loop(0, negs // GATHER_UNROLL, gather_negs, 0)
    n_even, n_odd = halves(0, negs)
    n_bf[:, 0:LANES] = n_rows[n_even, :].astype(BF16)
    n_bf[:, LANES:2 * LANES] = n_rows[n_odd, :].astype(BF16)

    def gather_tails(part, _):
        for off in range(GATHER_UNROLL):
            at = part * GATHER_UNROLL + off
            t_rows[pair(at), :] = table[tail_ids[0, at]]
        return 0

    lax.fori_loop(0, edges // GATHER_UNROLL, gather_tails, 0)

    gn_acc[...] = jnp.zeros_like(gn_acc)
    eye = lax.broadcasted_iota(jnp.int32, (LANES, LANES), 0) == lax.broadcasted_iota(jnp.int32, (LANES, LANES), 1)
    per_block = EDGE_BLOCK // LANES

    def answer(step, loss_acc):
        if shift:
            q_copy(step).wait_recv()
        even, odd = halves(step * EDGE_BLOCK, EDGE_BLOCK)
        if shift:
            wide = unpack_rows(used, 2 * EDGE_BLOCK, q_got[wire(step), :].astype(F32))
            q = jnp.concatenate([wide[:EDGE_BLOCK], wide[EDGE_BLOCK:]], axis=1).astype(BF16)
        else:
            q = q_own[block(step), :]
        t = jnp.concatenate([t_rows[even, :].astype(BF16), t_rows[odd, :].astype(BF16)], axis=1).astype(F32)
        q_wide = q.astype(F32)
        n = n_bf[...]
        masks = [tail_vec[0:1, pl.ds(pl.multiple_of(edges + step * EDGE_BLOCK + k * LANES, LANES), LANES)].astype(F32) for k in range(per_block)]
        w = jnp.concatenate([jnp.sum(jnp.where(eye, mask, 0.0), axis=1, keepdims=True) for mask in masks], axis=0)
        pos = jnp.sum(q_wide * t, axis=1, keepdims=True)
        score = lax.dot_general(q, n, (((1,), (1,)), ((), ())), preferred_element_type=F32)
        top = jnp.maximum(jnp.max(score, axis=1, keepdims=True), pos)
        pos_exp = jnp.exp(pos - top)
        neg_exp = jnp.exp(score - top)
        total = pos_exp + jnp.sum(neg_exp, axis=1, keepdims=True)
        loss_acc = loss_acc + jnp.sum(w * (top + jnp.log(total) - pos), axis=0, keepdims=True)
        d_pos = w * (pos_exp / total - 1.0)
        d_neg = ((w / total) * neg_exp).astype(BF16)
        g_q = d_pos * t + jnp.dot(d_neg, n, preferred_element_type=F32)
        g_tail = d_pos * q_wide
        gt_ref[even, :] = g_tail[:, 0:LANES]
        gt_ref[odd, :] = g_tail[:, LANES:2 * LANES]
        gn_acc[...] += lax.dot_general(q, d_neg, (((0,), (0,)), ((), ())), preferred_element_type=F32)
        if shift:
            gq_send[wire(step), :] = pack_rows(used, jnp.concatenate([g_q[:, 0:LANES], g_q[:, LANES:2 * LANES]], axis=0)).astype(BF16)
            gq_copy(step).start()
        else:
            gq_got[block(step), :] = g_q
        out_copy(gt_ref, gt_out, gt_sems, step).start()
        return loss_acc

    loss = lax.fori_loop(0, steps, answer, jnp.zeros((1, 1), F32))
    if shift:
        loss_send[...] = jnp.broadcast_to(loss, loss_send.shape)
        loss_copy = pltpu.make_async_remote_copy(
            src_ref=loss_send, dst_ref=loss_ref, send_sem=loss_sems.at[0], recv_sem=loss_sems.at[1],
            device_id={'ent': behind}, device_id_type=MESH)
        loss_copy.start()
    else:
        loss_ref[...] = jnp.broadcast_to(loss, loss_ref.shape)
    for half in range(2):
        gn_ref[pl.ds(half, negs, stride=2), :] = gn_acc[half * LANES:(half + 1) * LANES, :].T
    gn_copy.start()

    def finish(step, carry):
        rel_re, rel_im = carry
        if shift:
            gq_copy(step).wait_recv()
            wide = unpack_rows(used, 2 * EDGE_BLOCK, gq_got[wire(step), :].astype(F32))
            re_g, im_g = wide[:EDGE_BLOCK], wide[EDGE_BLOCK:]
        else:
            re_g, im_g = gq_got[block(step), 0:LANES], gq_got[block(step), LANES:2 * LANES]
        even, odd = halves(step * EDGE_BLOCK, EDGE_BLOCK)
        re_r, im_r = r_rows[even, :], r_rows[odd, :]
        gh_ref[even, :] = re_g * re_r + im_g * im_r
        gh_ref[odd, :] = im_g * re_r - re_g * im_r
        out_copy(gh_ref, gh_out, gh_sems, step).start()
        re_h, im_h = h_rows[even, :], h_rows[odd, :]
        ids = head_vec[0:1, pl.ds(pl.multiple_of(edges + step * EDGE_BLOCK, EDGE_BLOCK), EDGE_BLOCK)]
        hot = (lax.broadcasted_iota(jnp.int32, (rel_pad, EDGE_BLOCK), 0) == ids).astype(F32)
        rel_re = rel_re + jnp.dot(hot, re_g * re_h + im_g * im_h, precision=lax.Precision.HIGHEST, preferred_element_type=F32)
        rel_im = rel_im + jnp.dot(hot, im_g * re_h - re_g * im_h, precision=lax.Precision.HIGHEST, preferred_element_type=F32)
        return rel_re, rel_im

    zero = jnp.zeros((rel_pad, LANES), F32)
    rel_re, rel_im = lax.fori_loop(0, steps, finish, (zero, zero))
    grel_ref[pl.ds(0, rel_pad, stride=2), :] = rel_re
    grel_ref[pl.ds(1, rel_pad, stride=2), :] = rel_im
    if shift:
        loss_copy.wait()
    gn_copy.wait()

    def drain(step, _):
        if shift:
            q_copy(step).wait_send()
            gq_copy(step).wait_send()
        out_copy(gt_ref, gt_out, gt_sems, step).wait()
        out_copy(gh_ref, gh_out, gh_sems, step).wait()
        return 0

    lax.fori_loop(0, steps, drain, 0)


def scatter_kernel(head_ids, tail_ids, gh_in, gt_in, gn_in, acc_out, acc, acc_b, acc_c, acc_d, gh, gt_ref, gn_ref, in_sems, out_sems):
    edges = gh.shape[0] // 2
    negs = gn_ref.shape[0] // 2
    table_rows = acc.shape[0]
    zero_rows = 512
    pieces = 8
    piece = table_rows // pieces

    copies = [pltpu.make_async_copy(src, dst, in_sems.at[at]) for at, (src, dst) in enumerate(((gh_in, gh), (gt_in, gt_ref), (gn_in, gn_ref)))]
    for copy in copies:
        copy.start()

    def clear(step, _):
        rows = pl.ds(pl.multiple_of(step * zero_rows, zero_rows), zero_rows)
        for ref in (acc, acc_b, acc_c, acc_d):
            ref[rows, :] = jnp.zeros((zero_rows, LANES), F32)
        return 0

    lax.fori_loop(0, table_rows // zero_rows, clear, 0)
    for copy in copies:
        copy.wait()

    def add_edges(step, _):
        base = step * SCATTER_UNROLL
        for off in range(0, SCATTER_UNROLL, 2):
            at = base + off
            places = (pair(head_ids[0, at]), pair(head_ids[0, at + 1]), pair(tail_ids[0, at]), pair(tail_ids[0, at + 1]))
            refs = (acc, acc_b, acc_c, acc_d)
            terms = (gh[pair(at), :], gh[pair(at + 1), :], gt_ref[pair(at), :], gt_ref[pair(at + 1), :])
            sums = [ref[place, :] + term for ref, place, term in zip(refs, places, terms)]
            for ref, place, total in zip(refs, places, sums):
                ref[place, :] = total
        return 0

    lax.fori_loop(0, edges // SCATTER_UNROLL, add_edges, 0)

    def add_negs(step, _):
        base = step * SCATTER_UNROLL
        for off in range(0, SCATTER_UNROLL, 4):
            at = base + off
            places = [pair(tail_ids[0, 2 * edges + at + k]) for k in range(4)]
            refs = (acc, acc_b, acc_c, acc_d)
            sums = [ref[place, :] + gn_ref[pair(at + k), :] for k, (ref, place) in enumerate(zip(refs, places))]
            for ref, place, total in zip(refs, places, sums):
                ref[place, :] = total
        return 0

    lax.fori_loop(0, negs // SCATTER_UNROLL, add_negs, 0)

    def out_copy(at):
        rows = pl.ds(pl.multiple_of(at * piece, piece), piece)
        return pltpu.make_async_copy(acc.at[rows, :], acc_out.at[rows, :], out_sems.at[at])

    def combine(at, _):
        rows = pl.ds(pl.multiple_of(at * piece, piece), piece)
        acc[rows, :] = (acc[rows, :] + acc_b[rows, :]) + (acc_c[rows, :] + acc_d[rows, :])
        out_copy(at).start()
        return 0

    lax.fori_loop(0, pieces, combine, 0)
    for at in range(pieces):
        out_copy(at).wait()


def pieces_of(half):
    found, at = [], 0
    for bit in range(7, -1, -1):
        if half >> bit & 1:
            found.append((1 << bit, at))
            at += 1 << bit
    return found


def pack_rows(half, x):
    n = x.shape[0]
    lane = lax.broadcasted_iota(jnp.int32, (1, LANES), 1)
    out = []
    for size, at in pieces_of(half):
        groups = LANES // size
        rows = n // groups
        acc = None
        for k in range(groups):
            part = pltpu.roll(x[k * rows:(k + 1) * rows], (k * size - at) % LANES, 1)
            acc = part if acc is None else jnp.where(lane < k * size, acc, part)
        out.append(acc)
    return jnp.concatenate(out, axis=0)


def unpack_rows(half, n, x):
    lane = lax.broadcasted_iota(jnp.int32, (1, LANES), 1)
    out, start = None, 0
    for size, at in pieces_of(half):
        groups = LANES // size
        rows = n // groups
        block = x[start:start + rows]
        start += rows
        parts = jnp.concatenate([pltpu.roll(block, (at - k * size) % LANES, 1) for k in range(groups)], axis=0)
        out = parts if out is None else jnp.where(lane < at, out, parts)
    return jnp.where(lane < half, out, 0.0)


def update_kernel(width, learn_rate, groups, reps, shift, bucket_edges, acc_hbm, table_hbm, state_in, grel_in, rel_in, rel_state_in, loss_in, losses_in,
                  table_out, state_out, rel_out, rel_state_out, losses_out, state_all,
                  acc, table, first_send, first_got, plain_send, plain_got, merged_send, merged_got, work,
                  step_own, step_got, step_far, rel_x, rel_y, rel_send, rel_send_y, state_own, acc_sems, table_sems, out_sems,
                  first_sems, plain_sems, merged_sems, own_sems, far_sems, rel_x_sems, rel_y_sems, state_sems):
    me = lax.axis_index('data')
    ent = lax.axis_index('ent')
    used = width // 2
    peers = (lax.rem(me + 1, reps), lax.rem(me + reps - 1, reps))
    peer_slots = (1, reps - 1)
    half = acc.shape[2]
    chunk = half // SYNC_CHUNKS
    sent = chunk * used // LANES

    def part_rows(slot, which):
        return pl.ds(pl.multiple_of((lax.rem(me + slot, reps) * 2 + which) * half, half), half)

    def load(src, dst, sems, slot, which):
        return pltpu.make_async_copy(src.at[part_rows(slot, which), :], dst.at[slot, which], sems.at[slot, which])

    def save(slot, which):
        return pltpu.make_async_copy(table.at[slot, which], table_out.at[part_rows(slot, which), :], out_sems.at[slot, which])

    for slot, which in ((2, 0), (2, 1), (1, 1), (3, 0), (1, 0), (3, 1), (0, 0), (0, 1)):
        load(acc_hbm, acc, acc_sems, slot, which).start()
    for slot in range(reps):
        for which in range(2):
            load(table_hbm, table, table_sems, slot, which).start()

    barrier = pltpu.get_barrier_semaphore()
    for off in range(1, reps):
        pl.semaphore_signal(barrier, inc=1, device_id={'data': lax.rem(me + off, reps)}, device_id_type=MESH)
    for off in range(1, groups):
        pl.semaphore_signal(barrier, inc=1, device_id={'ent': lax.rem(ent + off, groups)}, device_id_type=MESH)
    pl.semaphore_wait(barrier, reps + groups - 2)

    def remote(src, dst, sems, place, to):
        return pltpu.make_async_remote_copy(
            src_ref=src, dst_ref=dst, send_sem=sems.at[(0,) + place], recv_sem=sems.at[(1,) + place],
            device_id=to, device_id_type=MESH)

    rel_x[0] = grel_in[...]
    rel_send[...] = grel_in[...]
    x_copies = [remote(rel_send, rel_x.at[off], rel_x_sems, (off - 1,), {'ent': lax.rem(ent + off, groups)}) for off in range(1, groups)]
    for copy in x_copies:
        copy.start()

    def at_chunk(k):
        return pl.ds(pl.multiple_of(k * chunk, chunk), chunk)

    def at_sent(k):
        return pl.ds(pl.multiple_of(k * sent, sent), sent)

    def first(side, k):
        return remote(first_send.at[side, at_sent(k), :], first_got.at[side, at_sent(k), :], first_sems, (side, k), {'data': peers[side]})

    def plain(side, k):
        return remote(plain_send.at[side, at_sent(k), :], plain_got.at[side, at_sent(k), :], plain_sems, (side, k), {'data': peers[side]})

    def merged(side, k):
        return remote(merged_send.at[side, at_sent(k), :], merged_got.at[side, at_sent(k), :], merged_sems, (side, k), {'data': peers[side]})

    def own(side, which, k):
        return remote(step_own.at[which, at_sent(k), :], step_got.at[side, which, at_sent(k), :], own_sems, (side, which, k), {'data': peers[side]})

    def spread(side, k):
        return remote(step_got.at[side, side, at_sent(k), :], step_far.at[side, at_sent(k), :], far_sems, (side, k), {'data': peers[side]})

    def send_first(k, _):
        for side in range(2):
            first_send[side, at_sent(k), :] = pack_rows(used, acc[2, side, at_chunk(k), :]).astype(BF16)
            first(side, k).start()
        return 0

    def send_plain(k, _):
        for side in range(2):
            plain_send[side, at_sent(k), :] = pack_rows(used, acc[peer_slots[side], 1 - side, at_chunk(k), :]).astype(BF16)
            plain(side, k).start()
        return 0

    def send_merged(k, _):
        for side in range(2):
            first(side, k).wait_recv()
            merged_send[side, at_sent(k), :] = (first_got[side, at_sent(k), :].astype(F32) + pack_rows(used, acc[peer_slots[side], side, at_chunk(k), :])).astype(BF16)
            merged(side, k).start()
        return 0

    for needed, body in ((((2, 0), (2, 1)), send_first), (((1, 1), (3, 0)), send_plain), (((1, 0), (3, 1)), send_merged)):
        for slot, which in needed:
            load(acc_hbm, acc, acc_sems, slot, which).wait()
        lax.fori_loop(0, SYNC_CHUNKS, body, 0)

    for copy in x_copies:
        copy.wait()
    total = rel_x[lax.rem(ent, groups)]
    for src in range(1, groups):
        total = total + rel_x[lax.rem(ent + groups - src, groups)]
    span = total.shape[0]
    rel_send_y[0:span, :] = total
    rel_send_y[span:, :] = loss_in[...]
    rel_y[0] = rel_send_y[...]
    y_copies = [remote(rel_send_y, rel_y.at[off], rel_y_sems, (off - 1,), {'data': lax.rem(me + off, reps)}) for off in range(1, reps)]
    for copy in y_copies:
        copy.start()

    for which in range(2):
        load(acc_hbm, acc, acc_sems, 0, which).wait()
    for slot in range(reps):
        for which in range(2):
            load(table_hbm, table, table_sems, slot, which).wait()
    n = chunk // 2
    even, odd = pl.ds(0, n, stride=2), pl.ds(1, n, stride=2)

    def step_rows(k, _):
        for which in range(2):
            merged(which, k).wait_recv()
            plain(1 - which, k).wait_recv()
            others = merged_got[which, at_sent(k), :].astype(F32) + plain_got[1 - which, at_sent(k), :].astype(F32)
            work[...] = acc[0, which, at_chunk(k), :] + unpack_rows(used, chunk, others)
            re_g, im_g = work[even, :], work[odd, :]
            places = pl.ds(pl.multiple_of(which * (half // 2) + k * n, n), n)
            state = state_in[places, :] + jnp.sum(re_g * re_g + im_g * im_g, axis=1, keepdims=True) / width
            state_out[places, :] = state
            scale = learn_rate / jnp.sqrt(state + EPSILON)
            work[even, :] = re_g * scale
            work[odd, :] = im_g * scale
            moves = work[...]
            step_own[which, at_sent(k), :] = pack_rows(used, moves).astype(BF16)
            for side in range(2):
                own(side, which, k).start()
            table[0, which, at_chunk(k), :] -= moves.astype(BF16).astype(F32)
        return 0

    lax.fori_loop(0, SYNC_CHUNKS, step_rows, 0)
    for which in range(2):
        save(0, which).start()

    def take_near(k, _):
        for which in range(2):
            for side in (which, 1 - which):
                own(side, which, k).wait_recv()
                if side == which:
                    spread(side, k).start()
                table[peer_slots[1 - side], which, at_chunk(k), :] -= unpack_rows(used, chunk, step_got[side, which, at_sent(k), :].astype(F32))
        return 0

    lax.fori_loop(0, SYNC_CHUNKS, take_near, 0)
    for slot in peer_slots:
        for which in range(2):
            save(slot, which).start()

    for copy in y_copies:
        copy.wait()
    total = rel_y[lax.rem(me, reps)]
    for src in range(1, reps):
        total = total + rel_y[lax.rem(me + reps - src, reps)]
    losses_out[...] = jnp.where(lax.broadcasted_iota(jnp.int32, losses_in.shape, 0) == shift, total[span:, :] / bucket_edges, losses_in[...])
    rel_send[...] = total[0:span, :]
    rel_rows = rel_send.shape[0] // 2
    re_g, im_g = rel_send[pl.ds(0, rel_rows, stride=2), :], rel_send[pl.ds(1, rel_rows, stride=2), :]
    state = rel_state_in[...] + jnp.sum(re_g * re_g + im_g * im_g, axis=1, keepdims=True) / width
    rel_state_out[...] = state
    scale = learn_rate / jnp.sqrt(state + EPSILON)
    rel_out[pl.ds(0, rel_rows, stride=2), :] = rel_in[pl.ds(0, rel_rows, stride=2), :] - re_g * scale
    rel_out[pl.ds(1, rel_rows, stride=2), :] = rel_in[pl.ds(1, rel_rows, stride=2), :] - im_g * scale

    state_copies = []
    if shift == groups - 1:
        eye = lax.broadcasted_iota(jnp.int32, (LANES, LANES), 0) == lax.broadcasted_iota(jnp.int32, (LANES, LANES), 1)
        blocks = state_own.shape[0]
        for at in range(blocks):
            state_own[at:at + 1, :] = jnp.sum(jnp.where(eye, state_out[at * LANES:(at + 1) * LANES, :], 0.0), axis=0, keepdims=True)
        place = pl.ds(pl.multiple_of(me * blocks, blocks), blocks)
        state_all[place, :] = state_own[...]
        state_copies = [remote(state_own, state_all.at[place, :], state_sems, (off - 1,), {'data': lax.rem(me + off, reps)}) for off in range(1, reps)]
        for copy in state_copies:
            copy.start()
    else:
        state_all[...] = jnp.zeros_like(state_all)

    def take_far(k, _):
        for side in range(2):
            spread(side, k).wait_recv()
            table[2, side, at_chunk(k), :] -= unpack_rows(used, chunk, step_far[side, at_sent(k), :].astype(F32))
        return 0

    lax.fori_loop(0, SYNC_CHUNKS, take_far, 0)
    for which in range(2):
        save(2, which).start()

    def drain(k, _):
        for side in range(2):
            for copy in (first(side, k), plain(side, k), merged(side, k), own(side, 0, k), own(side, 1, k), spread(side, k)):
                copy.wait_send()
        return 0

    lax.fori_loop(0, SYNC_CHUNKS, drain, 0)
    for slot in range(reps):
        for which in range(2):
            save(slot, which).wait()
    for copy in state_copies:
        copy.wait()


def solution(mesh):
    groups = mesh.shape['ent']
    reps = mesh.shape['data']
    row_spec = P(('sweep', 'ent'), None)
    edge_spec = P(('sweep', 'ent'), None, 'data')
    vmem = pl.BlockSpec(memory_space=VM)

    def device_fn(ent_table, ent_state, rel_table, head_idx, tail_idx, rel_idx, edge_mask, neg_idx):
        part_rows, width = ent_table.shape
        rel_count = rel_table.shape[0]
        edges = head_idx.shape[2]
        negs = neg_idx.shape[2]
        bucket_edges = edges * reps
        learn_rate = LR_SCALE * width ** -0.25
        rel_pad = -(-rel_count // 8) * 8
        quarter = part_rows // reps
        me = lax.axis_index('data')

        packed = jnp.concatenate([tail_idx[0], edge_mask[0], neg_idx[0]], axis=1)
        moved = [packed[0:1]]
        for shift in range(1, groups):
            moved.append(lax.ppermute(packed[shift:shift + 1], 'ent', [(src, (src + shift) % groups) for src in range(groups)]))

        owned = jnp.concatenate([head_idx[0], rel_idx[0]], axis=1)
        row_grid = 8
        params = pltpu.CompilerParams(vmem_limit_bytes=VMEM_LIMIT)
        table = pl.pallas_call(
            functools.partial(load_kernel, width // 2), grid=(row_grid,),
            out_shape=jax.ShapeDtypeStruct((2 * part_rows, LANES), F32),
            in_specs=[pl.BlockSpec((width, part_rows // row_grid), lambda i: (0, i))],
            out_specs=pl.BlockSpec((2 * part_rows // row_grid, LANES), lambda i: (i, 0)),
            scratch_shapes=[VM((2 * LANES, part_rows // row_grid), F32)], name='load_table')(ent_table.T)
        rel = interleave(jnp.pad(rel_table, ((0, rel_pad - rel_count), (0, 0))))
        rel_state = jnp.zeros((rel_pad, LANES), F32)
        state = jnp.broadcast_to(lax.dynamic_slice_in_dim(ent_state, me * quarter, quarter)[:, None], (quarter, LANES))
        losses = jnp.zeros((-(-groups // 8) * 8, LANES), F32)

        smem = pl.BlockSpec(memory_space=pltpu.SMEM)
        hbm = pl.BlockSpec(memory_space=pl.ANY)
        sems = pltpu.SemaphoreType.DMA
        steps = edges // EDGE_BLOCK
        for shift in range(groups):
            tail = moved[shift]
            head = owned[shift:shift + 1]
            scratch = [VM((part_rows, 2, LANES), F32)] + [VM((2 * edges, LANES), F32)] * 2 + [VM((2 * negs, LANES), F32)]
            scratch += [VM((2 * edges, LANES), F32)] * 3 + [VM((2 * negs, LANES), F32), VM((negs, 2 * LANES), BF16), VM((2 * LANES, negs), F32)]
            scratch += [sems((2,)), sems((steps,)), sems((steps,))]
            if shift:
                scratch += [VM((2 * edges * (width // 2) // LANES, LANES), BF16)] * 4 + [VM(losses.shape, F32), sems((2, steps)), sems((2, steps)), sems((2,))]
            else:
                scratch += [VM((edges, 2 * LANES), BF16), VM((edges, 2 * LANES), F32)]
            g_h, g_t, g_n, g_rel, loss = pl.pallas_call(
                functools.partial(bucket_kernel, shift, groups, width // 2),
                out_shape=[jax.ShapeDtypeStruct((2 * edges, LANES), F32)] * 2
                + [jax.ShapeDtypeStruct((2 * negs, LANES), F32), jax.ShapeDtypeStruct((2 * rel_pad, LANES), F32), jax.ShapeDtypeStruct(losses.shape, F32)],
                in_specs=[smem] * 2 + [hbm] + [vmem] * 3, out_specs=[hbm] * 3 + [vmem] * 2, scratch_shapes=scratch,
                compiler_params=pltpu.CompilerParams(vmem_limit_bytes=VMEM_LIMIT, collective_id=0, has_side_effects=True) if shift else params,
                name='bucket',
            )(head, tail, table.reshape(part_rows, 2, LANES), rel.reshape(rel_pad, 2, LANES), head, tail)

            acc = pl.pallas_call(
                scatter_kernel,
                out_shape=jax.ShapeDtypeStruct((2 * part_rows, LANES), F32),
                in_specs=[smem] * 2 + [hbm] * 3, out_specs=hbm,
                scratch_shapes=[VM((2 * part_rows, LANES), F32)] * 4 + [VM((2 * edges, LANES), F32)] * 2 + [VM((2 * negs, LANES), F32), sems((3,)), sems((8,))],
                compiler_params=params, name='scatter_rows',
            )(head, tail, g_h, g_t, g_n)

            half = (2 * part_rows) // reps // 2
            half_sent = half * (width // 2) // LANES
            block = VM((2, half_sent, LANES), BF16)
            state_blocks = quarter // LANES
            table, state, rel, rel_state, losses, state_all = pl.pallas_call(
                functools.partial(update_kernel, width, learn_rate, groups, reps, shift, bucket_edges),
                out_shape=[jax.ShapeDtypeStruct(table.shape, F32), jax.ShapeDtypeStruct(state.shape, F32),
                           jax.ShapeDtypeStruct(rel.shape, F32), jax.ShapeDtypeStruct(rel_state.shape, F32),
                           jax.ShapeDtypeStruct(losses.shape, F32), jax.ShapeDtypeStruct((reps * state_blocks, LANES), F32)],
                in_specs=[hbm] * 2 + [vmem] * 6, out_specs=[hbm] + [vmem] * 5,
                scratch_shapes=[VM((reps, 2, half, LANES), F32)] * 2 + [block] * 6 + [VM((half // SYNC_CHUNKS, LANES), F32), block, VM((2, 2, half_sent, LANES), BF16), block,
                                              VM((groups, 2 * rel_pad, LANES), F32), VM((reps, 2 * rel_pad + losses.shape[0], LANES), F32), VM((2 * rel_pad, LANES), F32),
                                              VM((2 * rel_pad + losses.shape[0], LANES), F32), VM((state_blocks, LANES), F32), sems((reps, 2)), sems((reps, 2)), sems((reps, 2)),
                                              sems((2, 2, SYNC_CHUNKS)), sems((2, 2, SYNC_CHUNKS)), sems((2, 2, SYNC_CHUNKS)),
                                              sems((2, 2, 2, SYNC_CHUNKS)), sems((2, 2, SYNC_CHUNKS)), sems((2, groups - 1)), sems((2, reps - 1)), sems((2, reps - 1))],
                compiler_params=pltpu.CompilerParams(vmem_limit_bytes=VMEM_LIMIT, collective_id=1, has_side_effects=True), name='update',
            )(acc, table, state, g_rel, rel, rel_state, loss, losses)

        ent_out = pl.pallas_call(
            functools.partial(store_kernel, width // 2), grid=(row_grid,),
            out_shape=jax.ShapeDtypeStruct((width, part_rows), F32),
            in_specs=[pl.BlockSpec((2 * part_rows // row_grid, LANES), lambda i: (i, 0))],
            out_specs=pl.BlockSpec((width, part_rows // row_grid), lambda i: (0, i)), name='store_table')(table).T
        rel_out = deinterleave(rel, width)[:rel_count]
        return ent_out, state_all.reshape(part_rows), rel_out, losses[:groups, 0].reshape(1, groups)

    return jax.shard_map(device_fn, mesh=mesh, in_specs=(row_spec, P(('sweep', 'ent')), P('sweep', None), edge_spec, edge_spec, edge_spec, edge_spec, P(('sweep', 'ent'), None, None)), out_specs=(row_spec, P(('sweep', 'ent')), P('sweep', None), row_spec), check_vma=False)
```
